32 devices in a mesh: member: 2 (over y), pts: 4 (over x, core), sub: 4 (over z).
Axes of the slice: x: 2, y: 2, z: 4, core: 2. Of those that a mesh axis runs over, the one named last changes fastest.
Arguments:
- spectrum: bfloat16 [1800, 32, 512], P(None, ('member', 'pts'), 'sub'), parts along dimension 1, may hold values from 0.049804688 to 2
- interaction: bfloat16 [1800, 1800], replicated, may hold values from -0.125 to 0.125
- speeds: float32 [1800], replicated, may hold values from 0.2 to 0.7
- mask: int32 [16, 512], P('pts', 'sub'), may hold values from 0 to 1, as said below
Outputs:
- evolved: bfloat16 [1800, 32, 512], P(None, ('member', 'pts'), 'sub'), parts along dimension 1
The draws below stay inside these ranges and needn't reach their ends.
There are 2 independent parts, one for each index of `member`. The reference program is written for one: setup_inputs(seed, part) draws one part's arguments, and reference() takes and returns one part's arrays. A program takes and returns all parts, laid end to end along the dimension named above; an argument that names none is the same for every part. Nothing has to cross between parts.
Inputs may be any that keep to these rules, and one draw needn't show every extreme that they name: `mask`: 1 marks sea, 0 land; the share of sea differs from grid row to grid row.
All inputs are finite; a program needn't handle non-finite values.
Results may differ from the reference program's by a relative error of at most 0.0075.
Values may be sent and summed in bfloat16 or wider, within the bound.
A program may use at most 128 MiB of HBM per device.

```python
import math
import jax
import jax.numpy as jnp

ND = 36
PROP = 2
K = 1800
GX = 16
GY = 512


def draw_mask(key, part):
    row_key, cell_key = jax.random.split(jax.random.fold_in(key, 17))
    level = jax.random.randint(row_key, (GX, 1), 30, 96)
    roll = jax.random.randint(cell_key, (GX, GY), 0, 100)
    return (roll < level).astype(jnp.int32)


def block_scale(stream_key, shape, shards, least, top_value):
    def one(axis_at, shards_of):
        heights = jax.random.uniform(jax.random.fold_in(jax.random.fold_in(stream_key, 6), axis_at), (shards_of,), jnp.float32, least / len(shards), top_value / len(shards))
        return jnp.repeat(jnp.exp(heights), shape[axis_at] // shards_of).reshape((-1,) + (1,) * (len(shape) - axis_at - 1))

    loudness = one(*shards[0])
    for cut in shards[1:]:
        loudness = loudness * one(*cut)
    return loudness


def normal_values(key, dims, scale, reach, kind=jnp.bfloat16):
    array = jax.random.normal(key, dims, jnp.float32) * scale
    return jnp.minimum(jnp.maximum(array, -reach), reach).astype(kind)


def setup_inputs(seed: int = 0, part: int = 0) -> dict:
    keys = jax.random.split(jax.random.key(seed), 5)
    own_keys = jax.random.split(jax.random.fold_in(keys[4], part), 5)
    spectrum = jnp.clip(0.049804688 + 1.9501953 * jax.random.uniform(own_keys[0], (K, GX, GY), jnp.float32) ** block_scale(own_keys[0], (K, GX, GY), ((1, 4), (2, 4)), -0.2, 0.2), 0.049804688, 2.0).astype(jnp.bfloat16)
    interaction = normal_values(keys[1], (K, K), K ** -0.5, 0.125)
    speeds = jnp.clip(jnp.exp(jax.random.uniform(keys[2], (K,), jnp.float32, math.log(0.2), math.log(0.7))), 0.2, 0.7)
    mask = draw_mask(jax.random.fold_in(keys[4], 71), part)
    return {"spectrum": spectrum, "interaction": interaction, "speeds": speeds, "mask": mask}


coupling = 0.5


def advance(field, cross, along, sea):
    cross_up = jnp.maximum(cross, 0.0)
    cross_down = jnp.minimum(cross, 0.0)
    along_up = jnp.maximum(along, 0.0)
    along_down = jnp.minimum(along, 0.0)
    for substep in range(PROP):
        ext = jnp.pad(field, ((0, 0), (1, 1), (1, 1)))
        back_x = ext[:, :-2, 1:-1]
        next_x = ext[:, 2:, 1:-1]
        back_y = ext[:, 1:-1, :-2]
        next_y = ext[:, 1:-1, 2:]
        field = (field - cross_up * (field - back_x) - cross_down * (next_x - field)
                 - along_up * (field - back_y) - along_down * (next_y - field)) * sea
    return field


def reference(spectrum, interaction, speeds, mask):
    flat = spectrum.reshape(K, GX * GY)
    coupled = jnp.dot(interaction, flat, preferred_element_type=jnp.float32)
    wide = flat.astype(jnp.float32)
    sea_flat = mask.astype(jnp.float32).reshape(1, GX * GY)
    grown = ((wide + coupling * wide * coupled) * sea_flat).astype(jnp.bfloat16).reshape(K, GX, GY)
    index = jnp.arange(K, dtype=jnp.int32)
    angle = (index % ND).astype(jnp.float32) * jnp.float32(2.0 * math.pi / ND)
    cross = (speeds * jnp.cos(angle)).reshape(K, 1, 1)
    along = (speeds * jnp.sin(angle)).reshape(K, 1, 1)
    field = advance(grown.astype(jnp.float32), cross, along, mask.astype(jnp.float32)[None])
    return field.astype(jnp.bfloat16)
```

```python
import functools
import math

import jax
import jax.numpy as jnp
import numpy as np
from jax import lax
from jax.experimental import pallas as pl
from jax.experimental.pallas import tpu as pltpu
from jax.sharding import PartitionSpec as P

ND = 36
PROP = 2
SUB = 16
UNIT = 72
PIECES = 9

coupling = 0.5


def circle():
    angle = np.arange(ND, dtype=np.int32).astype(np.float32) * np.float32(2.0 * math.pi / ND)
    angle = angle.astype(np.float64)
    return np.cos(angle).astype(np.float32), np.sin(angle).astype(np.float32)


def classes():
    cosine, sine = circle()
    key = [(bool(c > 0), bool(s >= 0)) for c, s in zip(cosine, sine)]
    first = next(d for d in range(ND) if key[d][0] and not key[d - 1][0])
    found = []
    for i in range(ND):
        d = (first + i) % ND
        if found and d > 0 and found[-1][0] == key[d]:
            found[-1][1].append(d)
        else:
            found.append((key[d], [d]))
    assert [k[0] for k, _ in found] == sorted((k[0] for k, _ in found), reverse=True)
    return found


def plan(comps):
    freqs = comps // ND
    groups, rest = freqs // SUB, freqs % SUB
    chunks = []
    for g in range(groups):
        main = [
            (g * SUB * ND + d, ND, SUB, up_x, up_y) for (up_x, up_y), run in classes() for d in run
        ]
        tail = []
        if g == groups - 1:
            tail = [
                ((groups * SUB + f) * ND + run[0], 1, len(run), up_x, up_y)
                for f in range(rest)
                for (up_x, up_y), run in classes()
            ]
            tail.sort(key=lambda t: t[0])
        tiles = [t for t in tail if t[3]] + main + [t for t in tail if not t[3]]
        ups = sum(t[3] for t in tiles)
        begin = g * SUB * ND
        end = comps if g == groups - 1 else begin + SUB * ND
        chunks.append((begin, end, tiles, ups))
    return chunks


def kernel(
    rows_x, chunks, counts,
    spec_hbm, inter_hbm, speeds_ref, mask_ref, stage,
    specv, inter, flat, acc, field, first, column, coefs, seas,
    xrecv, ysend, yrecv,
    load_sem, send_sem, recv_sem,
):
    comps, width = flat.shape
    lanes = width // rows_x
    f32, bf16 = jnp.float32, jnp.bfloat16
    px, sy = lax.axis_index("pts"), lax.axis_index("sub")
    nx, ny = counts
    partner = [{"pts": px + 1}, {"pts": px - 1}, {"sub": sy + 1}, {"sub": sy - 1}]
    sends = [px < nx - 1, px > 0, sy < ny - 1, sy > 0]
    receives = [sends[1], sends[0], sends[3], sends[2]]
    total = len(chunks)
    bases = list(np.cumsum([0] + [len(tiles) for _, _, tiles, _ in chunks]))

    spec_copy = pltpu.make_async_copy(spec_hbm, specv, load_sem.at[total])
    spec_copy.start()
    inter_copies = []
    for c, (begin, end, _, _) in enumerate(chunks):
        part = pl.ds(begin, end - begin)
        copy = pltpu.make_async_copy(inter_hbm.at[part], inter.at[part], load_sem.at[c])
        copy.start()
        inter_copies.append(copy)

    barrier = pltpu.get_barrier_semaphore()
    for kind in range(4):
        @pl.when(sends[kind])
        def _():
            pl.semaphore_signal(
                barrier, inc=1, device_id=partner[kind], device_id_type=pl.DeviceIdType.MESH
            )

    def exchange(e, c, kind):
        _, _, tiles, ups = chunks[c]
        if kind < 2:
            begin, count = (bases[c], ups) if kind == 0 else (bases[c] + ups, len(tiles) - ups)
            part = pl.ds(begin, count)
            source = (field if e == 0 else first).at[rows_x - 1 if kind == 0 else 0, part]
            target = xrecv.at[e, part]
        else:
            source, target = ysend.at[e, c], yrecv.at[e, kind - 2, c]
        return pltpu.make_async_remote_copy(
            src_ref=source, dst_ref=target,
            send_sem=send_sem.at[e, c, kind], recv_sem=recv_sem.at[e, c, kind],
            device_id=partner[kind], device_id_type=pl.DeviceIdType.MESH,
        )

    def start_sends(e, c):
        for kind in range(4):
            @pl.when(sends[kind])
            def _():
                exchange(e, c, kind).start()

    def wait_receives(e, c):
        for kind in range(4):
            @pl.when(receives[kind])
            def _():
                exchange(e, c, kind).wait_recv()

    for kind in range(2):
        @pl.when(jnp.logical_not(receives[kind]))
        def _():
            for e in range(PROP):
                for c, (_, _, tiles, ups) in enumerate(chunks):
                    begin, end = (0, ups) if kind == 0 else (ups, len(tiles))

                    @pl.loop(bases[c] + begin, bases[c] + end)
                    def _(t):
                        xrecv[e, t] = jnp.zeros(xrecv.shape[2:], bf16)

        @pl.when(jnp.logical_not(receives[kind + 2]))
        def _():
            for e in range(PROP):
                yrecv[e, kind] = jnp.zeros(yrecv.shape[2:], bf16)

    def lane_of(i, up_y):
        return 2 * i if up_y else 2 * i + 1

    starts = list(range(0, comps - lanes + 1, lanes))
    for at in starts:
        row = jnp.broadcast_to(speeds_ref[at : at + lanes].reshape(1, lanes), (lanes, lanes))
        column[at : at + lanes, :] = row.T
    done = starts[-1] + lanes
    if done < comps:
        row = jnp.broadcast_to(speeds_ref[done:comps].reshape(1, comps - done), (lanes, comps - done))
        column[done:comps, :] = row.T
    extra = column.shape[0] - comps
    column[comps : comps + extra, :] = jnp.zeros((extra, lanes), f32)
    stage[comps * rows_x : (comps + extra) * rows_x, :] = jnp.zeros((extra * rows_x, lanes), f32)

    cosine, sine = (np.abs(v) for v in circle())
    row_id = lax.broadcasted_iota(jnp.int32, (SUB, lanes), 0)
    for c, (_, _, tiles, _) in enumerate(chunks):
        for i, (k0, stride, real, _, _) in enumerate(tiles):
            speed = column[pl.ds(k0, SUB, stride=stride), :]
            if stride == 1:
                cx = jnp.zeros((SUB, lanes), f32)
                sx = jnp.zeros((SUB, lanes), f32)
                for r in range(real):
                    here = row_id == r
                    cx = jnp.where(here, float(cosine[(k0 + r) % ND]), cx)
                    sx = jnp.where(here, float(sine[(k0 + r) % ND]), sx)
                cross, along = speed * cx, speed * sx
            else:
                cross, along = speed * float(cosine[k0 % ND]), speed * float(sine[k0 % ND])
            coefs[bases[c] + i, 0] = 1.0 - cross - along
            coefs[bases[c] + i, 1] = cross
            coefs[bases[c] + i, 2] = along

    lane = lax.broadcasted_iota(jnp.int32, (SUB, lanes), 1)
    lane_f = lane.astype(f32).astype(bf16)
    parity = (lane % 2).astype(f32).astype(bf16)
    seaf = [
        jnp.broadcast_to(mask_ref[x : x + 1, :].astype(f32), (SUB, lanes)).astype(bf16)
        for x in range(rows_x)
    ]
    for i in range(seas.shape[0]):
        for x in range(rows_x):
            seas[i, x] = pltpu.roll(seaf[x], 2 * i + 1, 1)

    spec_copy.wait()

    small = mask_ref[...].astype(f32) * coupling
    sea_natural = jnp.concatenate([small] * (8 // rows_x), axis=0)

    def spread(block, count):
        length = count * UNIT
        begin = pl.multiple_of(block * (rows_x * UNIT), 16)
        whole = specv[pl.ds(begin, rows_x * length), :].astype(f32)
        whole = (whole.reshape(-1, 8, lanes) * sea_natural[None]).reshape(rows_x * length, lanes)
        stage[pl.ds(begin, rows_x * length), :] = whole
        for x in range(rows_x):
            values = stage[pl.ds(begin + x, length, stride=rows_x), :]
            flat[pl.ds(pl.multiple_of(block * UNIT, 8), length), x * lanes : (x + 1) * lanes] = (
                values.astype(bf16)
            )

    blocks = comps // UNIT

    @pl.loop(0, blocks // 2)
    def _(i):
        spread(2 * i, 2)

    if blocks % 2:
        spread(blocks - 1, 1)

    pl.semaphore_wait(barrier, sum(s.astype(jnp.int32) for s in sends))

    def grow(c):
        begin, end, tiles, _ = chunks[c]
        inter_copies[c].wait()
        product = jnp.dot(inter[begin:end, :], flat[...], preferred_element_type=f32)
        for x in range(rows_x):
            acc[x, 0 : end - begin, :] = product[:, x * lanes : (x + 1) * lanes]
        message = [jnp.zeros((SUB, lanes), bf16)] * rows_x
        for i, (k0, stride, _, _, up_y) in enumerate(tiles):
            mine = lane_f == float(lane_of(i, up_y))
            for x in range(rows_x):
                coupled = acc[x, pl.ds(k0 - begin, SUB, stride=stride), :]
                wide = stage[pl.ds(k0 * rows_x + x, SUB, stride=stride * rows_x), :]
                grown = (wide + wide * coupled).astype(bf16)
                grown = pltpu.roll(grown, 2 * i + 1, 1)
                field[x, bases[c] + i] = grown
                message[x] = jnp.where(mine, grown, message[x])
        for x in range(rows_x):
            ysend[0, c, x] = message[x]
        start_sends(0, c)

    def advance(e, c):
        _, _, tiles, _ = chunks[c]
        wait_receives(e, c)
        source = field if e == 0 else first
        even = parity == 0.0
        edges = [
            jnp.where(even, yrecv[e, 0, c, x], yrecv[e, 1, c, x]) for x in range(rows_x)
        ]
        message = [jnp.zeros((SUB, lanes), bf16)] * rows_x
        order = sorted(range(len(tiles)), key=lambda i: (tiles[i][1] == 1, tiles[i][0]))
        for i in order:
            k0, stride, _, up_x, up_y = tiles[i]
            t = bases[c] + i
            mine = lane_f == float(lane_of(i, up_y))
            keep, cross, along = (coefs[t, n].astype(bf16) for n in range(3))
            rows = [source[x, t] for x in range(rows_x)]
            outer = xrecv[e, t]
            for x in range(rows_x):
                if up_x:
                    near_x = rows[x - 1] if x > 0 else outer
                else:
                    near_x = rows[x + 1] if x < rows_x - 1 else outer
                near_y = pltpu.roll(
                    jnp.where(mine, edges[x], rows[x]), 1 if up_y else lanes - 1, 1
                )
                result = keep * rows[x] + cross * near_x + along * near_y
                if e == 0:
                    result = result * seas[i, x]
                    first[x, t] = result
                    message[x] = jnp.where(mine, result, message[x])
                else:
                    result = pltpu.roll(result, lanes - (2 * i + 1), 1)
                    stage[pl.ds(k0 * rows_x + x, SUB, stride=stride * rows_x), :] = (
                        result.astype(f32)
                    )
        if e == 0:
            for x in range(rows_x):
                ysend[1, c, x] = message[x]
            start_sends(1, c)

    for c in range(total):
        grow(c)
        if c >= 1:
            advance(0, c - 1)
    advance(0, total - 1)
    for c in range(total):
        advance(1, c)

    for e in range(PROP):
        for c in range(total):
            for kind in range(4):
                @pl.when(sends[kind])
                def _():
                    exchange(e, c, kind).wait_send()


def flush(rows_x, stage, mask_ref, out_hbm, outv, sem):
    lanes = outv.shape[1]
    piece = outv.shape[0] // PIECES
    twice = mask_ref[...].astype(jnp.float32) * (1.0 / coupling)
    sea = jnp.concatenate([twice] * (8 // rows_x), axis=0)
    copies = []
    for n in range(PIECES):
        part = pl.ds(n * piece, piece)
        values = stage[part, :].reshape(-1, 8, lanes) * sea[None]
        outv[part, :] = values.reshape(piece, lanes).astype(outv.dtype)
        copy = pltpu.make_async_copy(outv.at[part], out_hbm.at[part], sem.at[n])
        copy.start()
        copies.append(copy)
    for copy in copies:
        copy.wait()


def shards(mesh_counts, spectrum, interaction, speeds, mask):
    comps, rows_x, lanes = spectrum.shape
    chunks = plan(comps)
    total = len(chunks)
    tiles = sum(len(t) for _, _, t, _ in chunks)
    most = max(len(t) for _, _, t, _ in chunks)
    longest = max(end - begin for begin, end, _, _ in chunks)
    any_space = pl.BlockSpec(memory_space=pltpu.HBM)
    vmem = pl.BlockSpec(memory_space=pltpu.VMEM)
    f32, bf16 = jnp.float32, jnp.bfloat16
    stage = pl.pallas_call(
        functools.partial(kernel, rows_x, chunks, mesh_counts),
        out_shape=jax.ShapeDtypeStruct(((comps + SUB) * rows_x, lanes), f32),
        in_specs=[any_space, any_space, vmem, vmem],
        out_specs=vmem,
        scratch_shapes=[
            pltpu.VMEM((comps * rows_x, lanes), bf16),
            pltpu.VMEM((comps, comps), bf16),
            pltpu.VMEM((comps, rows_x * lanes), bf16),
            pltpu.VMEM((rows_x, longest + SUB, lanes), f32),
            pltpu.VMEM((rows_x, tiles, SUB, lanes), bf16),
            pltpu.VMEM((rows_x, tiles, SUB, lanes), bf16),
            pltpu.VMEM((comps + SUB, lanes), f32),
            pltpu.VMEM((tiles, 3, SUB, lanes), f32),
            pltpu.VMEM((most, rows_x, SUB, lanes), bf16),
            pltpu.VMEM((PROP, tiles, SUB, lanes), bf16),
            pltpu.VMEM((PROP, total, rows_x, SUB, lanes), bf16),
            pltpu.VMEM((PROP, 2, total, rows_x, SUB, lanes), bf16),
            pltpu.SemaphoreType.DMA((total + 1,)),
            pltpu.SemaphoreType.DMA((PROP, total, 4)),
            pltpu.SemaphoreType.DMA((PROP, total, 4)),
        ],
        compiler_params=pltpu.CompilerParams(
            collective_id=0, has_side_effects=True, vmem_limit_bytes=40 * 1024 * 1024
        ),
    )(spectrum.reshape(comps * rows_x, lanes), interaction, speeds, mask)
    out = pl.pallas_call(
        functools.partial(flush, rows_x),
        out_shape=jax.ShapeDtypeStruct((comps * rows_x, lanes), bf16),
        in_specs=[vmem, vmem],
        out_specs=any_space,
        scratch_shapes=[
            pltpu.VMEM((comps * rows_x, lanes), bf16),
            pltpu.SemaphoreType.DMA((PIECES,)),
        ],
        compiler_params=pltpu.CompilerParams(vmem_limit_bytes=12 * 1024 * 1024),
    )(stage, mask)
    return out.reshape(comps, rows_x, lanes)


def solution(mesh):
    placed = (P(None, ("member", "pts"), "sub"), P(), P(), P("pts", "sub"))
    return jax.shard_map(
        functools.partial(shards, (mesh.shape["pts"], mesh.shape["sub"])),
        mesh=mesh,
        in_specs=placed,
        out_specs=P(None, ("member", "pts"), "sub"),
        check_vma=False,
    )
```

```python
import functools
import math

import jax
import jax.numpy as jnp
import numpy as np
from jax import lax
from jax.experimental import pallas as pl
from jax.experimental.pallas import tpu as pltpu
from jax.sharding import PartitionSpec as P

ND = 36
PROP = 2
SUB = 16
PIECES = 10
PAD = 4

coupling = 0.5


def circle():
    angle = np.arange(ND, dtype=np.int32).astype(np.float32) * np.float32(2.0 * math.pi / ND)
    angle = angle.astype(np.float64)
    return np.cos(angle).astype(np.float32), np.sin(angle).astype(np.float32)


def classes():
    cosine, sine = circle()
    key = [(bool(c > 0), bool(s >= 0)) for c, s in zip(cosine, sine)]
    first = next(d for d in range(ND) if key[d][0] and not key[d - 1][0])
    found = []
    for i in range(ND):
        d = (first + i) % ND
        if found and d > 0 and found[-1][0] == key[d]:
            found[-1][1].append(d)
        else:
            found.append((key[d], [d]))
    assert [k[0] for k, _ in found] == sorted((k[0] for k, _ in found), reverse=True)
    return found


def plan(comps):
    freqs = comps // ND
    groups, rest = freqs // SUB, freqs % SUB
    chunks = []
    for g in range(groups):
        main = [
            (g * SUB * ND + d, ND, SUB, up_x, up_y) for (up_x, up_y), run in classes() for d in run
        ]
        tail = []
        if g == groups - 1:
            tail = [
                ((groups * SUB + f) * ND + run[0], 1, len(run), up_x, up_y)
                for f in range(rest)
                for (up_x, up_y), run in classes()
            ]
            tail.sort(key=lambda t: t[0])
        tiles = [t for t in tail if t[3]] + main + [t for t in tail if not t[3]]
        ups = sum(t[3] for t in tiles)
        begin = g * SUB * ND
        end = comps if g == groups - 1 else begin + SUB * ND
        chunks.append((begin, end, tiles, ups))
    return chunks


def pitch(rows_x):
    step = ND * rows_x + PAD
    return step if step % 8 else step + PAD


def kernel(
    rows_x, chunks, counts,
    spec_hbm, inter_hbm, speeds_hbm, mask_hbm, stage,
    speeds_ref, mask_ref, specv, inter, flat, acc, field, first, column, coefs, seas,
    xrecv, ysend, yrecv,
    load_sem, send_sem, recv_sem,
):
    comps, width = flat.shape
    lanes = width // rows_x
    f32, bf16 = jnp.float32, jnp.bfloat16
    px, sy = lax.axis_index("pts"), lax.axis_index("sub")
    nx, ny = counts
    partner = [{"pts": px + 1}, {"pts": px - 1}, {"sub": sy + 1}, {"sub": sy - 1}]
    sends = [px < nx - 1, px > 0, sy < ny - 1, sy > 0]
    receives = [sends[1], sends[0], sends[3], sends[2]]
    total = len(chunks)
    step = pitch(rows_x)
    bases = list(np.cumsum([0] + [len(tiles) for _, _, tiles, _ in chunks]))

    speeds_copy = pltpu.make_async_copy(speeds_hbm, speeds_ref, load_sem.at[total + 1])
    speeds_copy.start()
    mask_copy = pltpu.make_async_copy(mask_hbm, mask_ref, load_sem.at[total + 2])
    mask_copy.start()
    spec_copy = pltpu.make_async_copy(spec_hbm, specv, load_sem.at[total])
    spec_copy.start()
    inter_copies = []
    for c, (begin, end, _, _) in enumerate(chunks):
        part = pl.ds(begin, end - begin)
        copy = pltpu.make_async_copy(inter_hbm.at[part], inter.at[part], load_sem.at[c])
        copy.start()
        inter_copies.append(copy)

    barrier = pltpu.get_barrier_semaphore()
    for kind in range(4):
        @pl.when(sends[kind])
        def _():
            pl.semaphore_signal(
                barrier, inc=1, device_id=partner[kind], device_id_type=pl.DeviceIdType.MESH
            )

    def exchange(e, c, kind):
        _, _, tiles, ups = chunks[c]
        if kind < 2:
            begin, count = (bases[c], ups) if kind == 0 else (bases[c] + ups, len(tiles) - ups)
            part = pl.ds(begin, count)
            source = (field if e == 0 else first).at[rows_x - 1 if kind == 0 else 0, part]
            target = xrecv.at[e, part]
        else:
            source, target = ysend.at[e, c], yrecv.at[e, kind - 2, c]
        return pltpu.make_async_remote_copy(
            src_ref=source, dst_ref=target,
            send_sem=send_sem.at[e, c, kind], recv_sem=recv_sem.at[e, c, kind],
            device_id=partner[kind], device_id_type=pl.DeviceIdType.MESH,
        )

    def start_sends(e, c):
        for kind in range(4):
            @pl.when(sends[kind])
            def _():
                exchange(e, c, kind).start()

    def wait_receives(e, c):
        for kind in range(4):
            @pl.when(receives[kind])
            def _():
                exchange(e, c, kind).wait_recv()

    for kind in range(2):
        @pl.when(jnp.logical_not(receives[kind]))
        def _():
            for e in range(PROP):
                for c, (_, _, tiles, ups) in enumerate(chunks):
                    begin, end = (0, ups) if kind == 0 else (ups, len(tiles))

                    @pl.loop(bases[c] + begin, bases[c] + end)
                    def _(t):
                        xrecv[e, t] = jnp.zeros(xrecv.shape[2:], bf16)

        @pl.when(jnp.logical_not(receives[kind + 2]))
        def _():
            for e in range(PROP):
                yrecv[e, kind] = jnp.zeros(yrecv.shape[2:], bf16)

    def lane_of(i, up_y):
        return 2 * i if up_y else 2 * i + 1

    speeds_copy.wait()
    mask_copy.wait()

    starts = list(range(0, comps - lanes + 1, lanes))
    for at in starts:
        row = jnp.broadcast_to(speeds_ref[at : at + lanes].reshape(1, lanes), (lanes, lanes))
        column[at : at + lanes, :] = row.T
    done = starts[-1] + lanes
    if done < comps:
        row = jnp.broadcast_to(speeds_ref[done:comps].reshape(1, comps - done), (lanes, comps - done))
        column[done:comps, :] = row.T
    extra = column.shape[0] - comps
    column[comps : comps + extra, :] = jnp.zeros((extra, lanes), f32)
    used = comps // ND * step
    stage[used:, :] = jnp.zeros((stage.shape[0] - used, lanes), f32)
    stage[stage.shape[0] - 8 :, :] = jnp.concatenate(
        [mask_ref[...].astype(f32) * (1.0 / coupling)] * (8 // rows_x), axis=0
    )

    cosine, sine = (np.abs(v) for v in circle())
    row_id = lax.broadcasted_iota(jnp.int32, (SUB, lanes), 0)
    for c, (_, _, tiles, _) in enumerate(chunks):
        for i, (k0, stride, real, _, _) in enumerate(tiles):
            speed = column[pl.ds(k0, SUB, stride=stride), :]
            if stride == 1:
                cx = jnp.zeros((SUB, lanes), f32)
                sx = jnp.zeros((SUB, lanes), f32)
                for r in range(real):
                    here = row_id == r
                    cx = jnp.where(here, float(cosine[(k0 + r) % ND]), cx)
                    sx = jnp.where(here, float(sine[(k0 + r) % ND]), sx)
                cross, along = speed * cx, speed * sx
            else:
                cross, along = speed * float(cosine[k0 % ND]), speed * float(sine[k0 % ND])
            coefs[bases[c] + i, 0] = 1.0 - cross - along
            coefs[bases[c] + i, 1] = cross
            coefs[bases[c] + i, 2] = along

    lane = lax.broadcasted_iota(jnp.int32, (SUB, lanes), 1)
    lane_f = lane.astype(f32).astype(bf16)
    parity = (lane % 2).astype(f32).astype(bf16)
    seaf = [
        jnp.broadcast_to(mask_ref[x : x + 1, :].astype(f32), (SUB, lanes)).astype(bf16)
        for x in range(rows_x)
    ]
    for i in range(seas.shape[0]):
        for x in range(rows_x):
            seas[i, x] = pltpu.roll(seaf[x], 2 * i + 1, 1)

    spec_copy.wait()

    small = mask_ref[...].astype(f32) * coupling
    sea_natural = jnp.concatenate([small] * (8 // rows_x), axis=0)

    low = lax.broadcasted_iota(jnp.int32, (8, lanes), 0) < ND % 8
    whole_rows = ND // 8 * 8

    @pl.loop(0, comps // (2 * ND))
    def _(block):
        length = ND * rows_x
        begin = pl.multiple_of(block * (2 * length), 16)
        home = pl.multiple_of(block * (2 * step), 8)
        values = specv[pl.ds(begin, 2 * length), :].astype(f32)
        values = (values.reshape(-1, 8, lanes) * sea_natural[None]).reshape(2 * length, lanes)
        stage[pl.ds(home, length), :] = values[:length]
        stage[pl.ds(home + step, length), :] = values[length:]
        for x in range(rows_x):
            one = stage[pl.ds(home + x, whole_rows + 8, stride=rows_x), :]
            two = stage[pl.ds(home + step - ND % 8 * rows_x + x, whole_rows + 8, stride=rows_x), :]
            middle = jnp.where(low, one[whole_rows:], two[:8])
            both = jnp.concatenate([one[:whole_rows], middle, two[8:]], axis=0)
            flat[pl.ds(pl.multiple_of(block * (2 * ND), 8), 2 * ND), x * lanes : (x + 1) * lanes] = (
                both.astype(bf16)
            )

    pl.semaphore_wait(barrier, sum(s.astype(jnp.int32) for s in sends))

    def staged(k0, stride, x):
        begin = k0 // ND * step + k0 % ND * rows_x + x
        return pl.ds(begin, SUB, stride=rows_x if stride == 1 else step)

    def grow(c):
        begin, end, tiles, _ = chunks[c]
        inter_copies[c].wait()
        product = jnp.dot(inter[begin:end, :], flat[...], preferred_element_type=f32)
        for x in range(rows_x):
            acc[x, 0 : end - begin, :] = product[:, x * lanes : (x + 1) * lanes]
        message = [jnp.zeros((SUB, lanes), bf16)] * rows_x
        for i, (k0, stride, _, _, up_y) in enumerate(tiles):
            mine = lane_f == float(lane_of(i, up_y))
            for x in range(rows_x):
                coupled = acc[x, pl.ds(k0 - begin, SUB, stride=stride), :]
                wide = stage[staged(k0, stride, x), :]
                grown = (wide + wide * coupled).astype(bf16)
                grown = pltpu.roll(grown, 2 * i + 1, 1)
                field[x, bases[c] + i] = grown
                message[x] = jnp.where(mine, grown, message[x])
        for x in range(rows_x):
            ysend[0, c, x] = message[x]
        start_sends(0, c)

    def advance(e, c):
        _, _, tiles, _ = chunks[c]
        wait_receives(e, c)
        source = field if e == 0 else first
        even = parity == 0.0
        edges = [
            jnp.where(even, yrecv[e, 0, c, x], yrecv[e, 1, c, x]) for x in range(rows_x)
        ]
        message = [jnp.zeros((SUB, lanes), bf16)] * rows_x
        order = sorted(range(len(tiles)), key=lambda i: (tiles[i][1] == 1, tiles[i][0]))
        for i in order:
            k0, stride, _, up_x, up_y = tiles[i]
            t = bases[c] + i
            mine = lane_f == float(lane_of(i, up_y))
            keep, cross, along = (coefs[t, n].astype(bf16) for n in range(3))
            rows = [source[x, t] for x in range(rows_x)]
            outer = xrecv[e, t]
            for x in range(rows_x):
                if up_x:
                    near_x = rows[x - 1] if x > 0 else outer
                else:
                    near_x = rows[x + 1] if x < rows_x - 1 else outer
                near_y = pltpu.roll(
                    jnp.where(mine, edges[x], rows[x]), 1 if up_y else lanes - 1, 1
                )
                result = keep * rows[x] + cross * near_x + along * near_y
                if e == 0:
                    result = result * seas[i, x]
                    first[x, t] = result
                    message[x] = jnp.where(mine, result, message[x])
                else:
                    result = pltpu.roll(result, lanes - (2 * i + 1), 1)
                    stage[staged(k0, stride, x), :] = result.astype(f32)
        if e == 0:
            for x in range(rows_x):
                ysend[1, c, x] = message[x]
            start_sends(1, c)

    for c in range(total):
        grow(c)
        if c >= 1:
            advance(0, c - 1)
    advance(0, total - 1)
    for c in range(total):
        advance(1, c)

    for e in range(PROP):
        for c in range(total):
            for kind in range(4):
                @pl.when(sends[kind])
                def _():
                    exchange(e, c, kind).wait_send()


def flush(rows_x, stage, out_hbm, outv, sem):
    lanes = outv.shape[1]
    length, step = ND * rows_x, pitch(rows_x)
    freqs = outv.shape[0] // length
    pieces = sem.shape[0]
    each = freqs // pieces
    sea = stage[stage.shape[0] - 8 :, :]
    copies = []
    for n in range(pieces):
        for f in range(n * each, (n + 1) * each):
            values = stage[f * step : f * step + length, :].reshape(-1, 8, lanes) * sea[None]
            outv[f * length : (f + 1) * length, :] = values.reshape(length, lanes).astype(outv.dtype)
        part = pl.ds(n * each * length, each * length)
        copy = pltpu.make_async_copy(outv.at[part], out_hbm.at[part], sem.at[n])
        copy.start()
        copies.append(copy)
    for copy in copies:
        copy.wait()


def shards(mesh_counts, spectrum, interaction, speeds, mask):
    comps, rows_x, lanes = spectrum.shape
    chunks = plan(comps)
    total = len(chunks)
    tiles = sum(len(t) for _, _, t, _ in chunks)
    most = max(len(t) for _, _, t, _ in chunks)
    longest = max(end - begin for begin, end, _, _ in chunks)
    any_space = pl.BlockSpec(memory_space=pltpu.HBM)
    vmem = pl.BlockSpec(memory_space=pltpu.VMEM)
    f32, bf16 = jnp.float32, jnp.bfloat16
    freqs = comps // ND
    pieces = next(n for n in range(PIECES, 0, -1) if freqs % n == 0)
    held = -(-(freqs * pitch(rows_x) + SUB * rows_x) // 8) * 8 + 8
    grant = 40 * 1024 * 1024
    pin = functools.partial(pltpu.with_memory_space_constraint, memory_space=pltpu.HBM)
    stage = pl.pallas_call(
        functools.partial(kernel, rows_x, chunks, mesh_counts),
        out_shape=jax.ShapeDtypeStruct((held, lanes), f32),
        in_specs=[any_space] * 4,
        out_specs=vmem,
        scratch_shapes=[
            pltpu.VMEM(speeds.shape, f32),
            pltpu.VMEM(mask.shape, mask.dtype),
            pltpu.VMEM((comps * rows_x, lanes), bf16),
            pltpu.VMEM((comps, comps), bf16),
            pltpu.VMEM((comps, rows_x * lanes), bf16),
            pltpu.VMEM((rows_x, longest + SUB, lanes), f32),
            pltpu.VMEM((rows_x, tiles, SUB, lanes), bf16),
            pltpu.VMEM((rows_x, tiles, SUB, lanes), bf16),
            pltpu.VMEM((comps + SUB, lanes), f32),
            pltpu.VMEM((tiles, 3, SUB, lanes), f32),
            pltpu.VMEM((most, rows_x, SUB, lanes), bf16),
            pltpu.VMEM((PROP, tiles, SUB, lanes), bf16),
            pltpu.VMEM((PROP, total, rows_x, SUB, lanes), bf16),
            pltpu.VMEM((PROP, 2, total, rows_x, SUB, lanes), bf16),
            pltpu.SemaphoreType.DMA((total + 3,)),
            pltpu.SemaphoreType.DMA((PROP, total, 4)),
            pltpu.SemaphoreType.DMA((PROP, total, 4)),
        ],
        compiler_params=pltpu.CompilerParams(
            collective_id=0, has_side_effects=True, vmem_limit_bytes=grant
        ),
    )(pin(spectrum.reshape(comps * rows_x, lanes)), pin(interaction), pin(speeds), pin(mask))
    out = pl.pallas_call(
        functools.partial(flush, rows_x),
        out_shape=jax.ShapeDtypeStruct((comps * rows_x, lanes), bf16),
        in_specs=[vmem],
        out_specs=any_space,
        scratch_shapes=[
            pltpu.VMEM((comps * rows_x, lanes), bf16),
            pltpu.SemaphoreType.DMA((pieces,)),
        ],
        compiler_params=pltpu.CompilerParams(vmem_limit_bytes=12 * 1024 * 1024),
    )(stage)
    return out.reshape(comps, rows_x, lanes)


def solution(mesh):
    placed = (P(None, ("member", "pts"), "sub"), P(), P(), P("pts", "sub"))
    return jax.shard_map(
        functools.partial(shards, (mesh.shape["pts"], mesh.shape["sub"])),
        mesh=mesh,
        in_specs=placed,
        out_specs=P(None, ("member", "pts"), "sub"),
        check_vma=False,
    )
```

```python
import functools
import math

import jax
import jax.numpy as jnp
import numpy as np
from jax import lax
from jax.experimental import pallas as pl
from jax.experimental.pallas import tpu as pltpu
from jax.sharding import PartitionSpec as P

ND = 36
PROP = 2
SUB = 16
HALF = 8
SIZES = (1, 2, 2, 1)
LAG = 3
LOADS = 5
PIECES = 10
PAD = 4

coupling = 0.5


def circle():
    angle = np.arange(ND, dtype=np.int32).astype(np.float32) * np.float32(2.0 * math.pi / ND)
    angle = angle.astype(np.float64)
    return np.cos(angle).astype(np.float32), np.sin(angle).astype(np.float32)


def classes():
    cosine, sine = circle()
    key = [(bool(c > 0), bool(s >= 0)) for c, s in zip(cosine, sine)]
    first = next(d for d in range(ND) if key[d][0] and not key[d - 1][0])
    found = []
    for i in range(ND):
        d = (first + i) % ND
        if found and d > 0 and found[-1][0] == key[d]:
            found[-1][1].append(d)
        else:
            found.append((key[d], [d]))
    assert [k[0] for k, _ in found] == sorted((k[0] for k, _ in found), reverse=True)
    return found


def plan(comps):
    freqs = comps // ND
    groups, rest = freqs // HALF, freqs % HALF
    sizes, left = [], groups
    for size in SIZES:
        size = min(size, left)
        if size:
            sizes.append(size)
            left -= size
    while left:
        sizes.insert(1, min(2, left))
        left -= sizes[1]
    chunks, top = [], groups
    for n, size in enumerate(sizes):
        tiles = []
        for g in range(top - size, top):
            for (up_x, up_y), run in classes():
                for pair in [run[i : i + 2] for i in range(0, len(run), 2)]:
                    pair = (pair * 2)[:2]
                    tiles.append(([(g * HALF * ND + d, ND, [d] * HALF) for d in pair], up_x, up_y))
        begin, end = (top - size) * HALF * ND, top * HALF * ND
        if n == 0:
            end = comps
            for f in range(rest):
                for (up_x, up_y), run in sorted(classes(), key=lambda c: c[1][0]):
                    ds = run + [None] * (SUB - len(run))
                    k0 = (groups * HALF + f) * ND + run[0]
                    parts = [(k0, 1, ds[:HALF]), (k0 + HALF, 1, ds[HALF:])]
                    tiles.append((parts, up_x, up_y))
        tiles.sort(key=lambda t: not t[1])
        chunks.append((begin, end, tiles, sum(t[1] for t in tiles)))
        top -= size
    return chunks


def pitch(rows_x):
    step = ND * rows_x + PAD
    return step if step % 8 else step + PAD


def kernel(
    rows_x, chunks, counts,
    spec_hbm, inter_hbm, speeds_hbm, mask_hbm, stage,
    speeds_ref, mask_ref, specv, inter, flat, acc, field, first, column, coefs, seas,
    xrecv, ysend, yrecv,
    load_sem, send_sem, recv_sem,
):
    comps, width = flat.shape
    lanes = width // rows_x
    f32, bf16 = jnp.float32, jnp.bfloat16
    px, sy = lax.axis_index("pts"), lax.axis_index("sub")
    nx, ny = counts
    partner = [{"pts": px + 1}, {"pts": px - 1}, {"sub": sy + 1}, {"sub": sy - 1}]
    sends = [px < nx - 1, px > 0, sy < ny - 1, sy > 0]
    receives = [sends[1], sends[0], sends[3], sends[2]]
    total = len(chunks)
    step = pitch(rows_x)
    bases = list(np.cumsum([0] + [len(tiles) for _, _, tiles, _ in chunks]))

    speeds_copy = pltpu.make_async_copy(speeds_hbm, speeds_ref, load_sem.at[total])
    speeds_copy.start()
    mask_copy = pltpu.make_async_copy(mask_hbm, mask_ref, load_sem.at[total + 1])
    mask_copy.start()
    blocks = comps // (2 * ND)
    loads = next(n for n in range(LOADS, 0, -1) if blocks % n == 0)
    piece = comps * rows_x // loads

    def spec_copy(n):
        part = pl.ds(pl.multiple_of(n * piece, 16), piece)
        return pltpu.make_async_copy(spec_hbm.at[part], specv.at[part], load_sem.at[total + 2 + n])

    for n in range(loads):
        spec_copy(n).start()
    inter_copies = []
    for c, (begin, end, _, _) in enumerate(chunks):
        part = pl.ds(begin, end - begin)
        copy = pltpu.make_async_copy(inter_hbm.at[part], inter.at[part], load_sem.at[c])
        copy.start()
        inter_copies.append(copy)

    barrier = pltpu.get_barrier_semaphore()
    for kind in range(4):
        @pl.when(sends[kind])
        def _():
            pl.semaphore_signal(
                barrier, inc=1, device_id=partner[kind], device_id_type=pl.DeviceIdType.MESH
            )

    def exchange(e, c, kind):
        _, _, tiles, ups = chunks[c]
        if kind < 2:
            begin, count = (bases[c], ups) if kind == 0 else (bases[c] + ups, len(tiles) - ups)
            part = pl.ds(begin, count)
            source = (field if e == 0 else first).at[rows_x - 1 if kind == 0 else 0, part]
            target = xrecv.at[e, part]
        else:
            source, target = ysend.at[e, c], yrecv.at[e, kind - 2, c]
        return pltpu.make_async_remote_copy(
            src_ref=source, dst_ref=target,
            send_sem=send_sem.at[e, c, kind], recv_sem=recv_sem.at[e, c, kind],
            device_id=partner[kind], device_id_type=pl.DeviceIdType.MESH,
        )

    def start_sends(e, c):
        for kind in range(4):
            @pl.when(sends[kind])
            def _():
                exchange(e, c, kind).start()

    def wait_receives(e, c):
        for kind in range(4):
            @pl.when(receives[kind])
            def _():
                exchange(e, c, kind).wait_recv()

    for kind in range(2):
        @pl.when(jnp.logical_not(receives[kind]))
        def _():
            for e in range(PROP):
                for c, (_, _, tiles, ups) in enumerate(chunks):
                    begin, end = (0, ups) if kind == 0 else (ups, len(tiles))

                    @pl.loop(bases[c] + begin, bases[c] + end)
                    def _(t):
                        xrecv[e, t] = jnp.zeros(xrecv.shape[2:], bf16)

        @pl.when(jnp.logical_not(receives[kind + 2]))
        def _():
            for e in range(PROP):
                yrecv[e, kind] = jnp.zeros(yrecv.shape[2:], bf16)

    def lane_of(i, up_y):
        return 2 * i if up_y else 2 * i + 1

    speeds_copy.wait()
    mask_copy.wait()

    starts = list(range(0, comps - lanes + 1, lanes))
    for at in starts:
        row = jnp.broadcast_to(speeds_ref[at : at + lanes].reshape(1, lanes), (lanes, lanes))
        column[at : at + lanes, :] = row.T
    done = starts[-1] + lanes
    if done < comps:
        row = jnp.broadcast_to(speeds_ref[done:comps].reshape(1, comps - done), (lanes, comps - done))
        column[done:comps, :] = row.T
    extra = column.shape[0] - comps
    column[comps : comps + extra, :] = jnp.zeros((extra, lanes), f32)
    used = comps // ND * step
    stage[used:, :] = jnp.zeros((stage.shape[0] - used, lanes), f32)
    stage[stage.shape[0] - 8 :, :] = jnp.concatenate(
        [mask_ref[...].astype(f32) * (1.0 / coupling)] * (8 // rows_x), axis=0
    )

    cosine, sine = (np.abs(v) for v in circle())
    row_id = lax.broadcasted_iota(jnp.int32, (HALF, lanes), 0)

    def factor(values, directions):
        found = [float(values[d]) if d is not None else 0.0 for d in directions]
        if len(set(found)) == 1:
            return found[0]
        column = jnp.zeros((HALF, lanes), f32)
        for r, value in enumerate(found):
            column = jnp.where(row_id == r, value, column)
        return column

    for c, (_, _, tiles, _) in enumerate(chunks):
        for i, (parts, _, _) in enumerate(tiles):
            for h, (k0, stride, directions) in enumerate(parts):
                rows = slice(h * HALF, (h + 1) * HALF)
                speed = column[pl.ds(k0, HALF, stride=stride), :]
                cross, along = speed * factor(cosine, directions), speed * factor(sine, directions)
                coefs[bases[c] + i, 0, rows] = 1.0 - cross - along
                coefs[bases[c] + i, 1, rows] = cross
                coefs[bases[c] + i, 2, rows] = along

    lane = lax.broadcasted_iota(jnp.int32, (SUB, lanes), 1)
    lane_f = lane.astype(f32).astype(bf16)
    parity = (lane % 2).astype(f32).astype(bf16)
    seaf = [
        jnp.broadcast_to(mask_ref[x : x + 1, :].astype(f32), (SUB, lanes)).astype(bf16)
        for x in range(rows_x)
    ]
    for i in range(seas.shape[0]):
        for x in range(rows_x):
            seas[i, x] = pltpu.roll(seaf[x], 2 * i + 1, 1)

    small = mask_ref[...].astype(f32) * coupling
    sea_natural = jnp.concatenate([small] * (8 // rows_x), axis=0)

    low = lax.broadcasted_iota(jnp.int32, (8, lanes), 0) < ND % 8
    whole_rows = ND // 8 * 8

    def spread(block):
        length = ND * rows_x
        begin = pl.multiple_of(block * (2 * length), 16)
        home = pl.multiple_of(block * (2 * step), 8)
        values = specv[pl.ds(begin, 2 * length), :].astype(f32)
        values = (values.reshape(-1, 8, lanes) * sea_natural[None]).reshape(2 * length, lanes)
        stage[pl.ds(home, length), :] = values[:length]
        stage[pl.ds(home + step, length), :] = values[length:]
        for x in range(rows_x):
            one = stage[pl.ds(home + x, whole_rows + 8, stride=rows_x), :]
            two = stage[pl.ds(home + step - ND % 8 * rows_x + x, whole_rows + 8, stride=rows_x), :]
            middle = jnp.where(low, one[whole_rows:], two[:8])
            both = jnp.concatenate([one[:whole_rows], middle, two[8:]], axis=0)
            flat[pl.ds(pl.multiple_of(block * (2 * ND), 8), 2 * ND), x * lanes : (x + 1) * lanes] = (
                both.astype(bf16)
            )

    @pl.loop(0, loads)
    def _(n):
        spec_copy(n).wait()
        for i in range(blocks // loads):
            spread(n * (blocks // loads) + i)

    pl.semaphore_wait(barrier, sum(s.astype(jnp.int32) for s in sends))

    def staged(part, x):
        k0, stride, _ = part
        begin = k0 // ND * step + k0 % ND * rows_x + x
        return pl.ds(begin, HALF, stride=rows_x if stride == 1 else step)

    def grow(c):
        begin, end, tiles, _ = chunks[c]
        inter_copies[c].wait()
        product = jnp.dot(inter[begin:end, :], flat[...], preferred_element_type=f32)
        for x in range(rows_x):
            acc[x, 0 : end - begin, :] = product[:, x * lanes : (x + 1) * lanes]
        message = [jnp.zeros((SUB, lanes), bf16)] * rows_x
        for i, (parts, _, up_y) in enumerate(tiles):
            mine = lane_f == float(lane_of(i, up_y))
            for x in range(rows_x):
                halves = []
                for part in parts:
                    k0, stride, _ = part
                    coupled = acc[x, pl.ds(k0 - begin, HALF, stride=stride), :]
                    wide = stage[staged(part, x), :]
                    halves.append(wide + wide * coupled)
                grown = jnp.concatenate(halves, axis=0).astype(bf16)
                grown = pltpu.roll(grown, 2 * i + 1, 1)
                field[x, bases[c] + i] = grown
                message[x] = jnp.where(mine, grown, message[x])
        for x in range(rows_x):
            ysend[0, c, x] = message[x]
        start_sends(0, c)

    def advance(e, c):
        _, _, tiles, _ = chunks[c]
        wait_receives(e, c)
        source = field if e == 0 else first
        even = parity == 0.0
        edges = [
            jnp.where(even, yrecv[e, 0, c, x], yrecv[e, 1, c, x]) for x in range(rows_x)
        ]
        message = [jnp.zeros((SUB, lanes), bf16)] * rows_x
        order = sorted(range(len(tiles)), key=lambda i: (tiles[i][0][0][1] == 1, tiles[i][0][0][0]))
        for i in order:
            parts, up_x, up_y = tiles[i]
            t = bases[c] + i
            mine = lane_f == float(lane_of(i, up_y))
            keep, cross, along = (coefs[t, n].astype(bf16) for n in range(3))
            rows = [source[x, t] for x in range(rows_x)]
            outer = xrecv[e, t]
            for x in range(rows_x):
                if up_x:
                    near_x = rows[x - 1] if x > 0 else outer
                else:
                    near_x = rows[x + 1] if x < rows_x - 1 else outer
                near_y = pltpu.roll(
                    jnp.where(mine, edges[x], rows[x]), 1 if up_y else lanes - 1, 1
                )
                result = keep * rows[x] + cross * near_x + along * near_y
                if e == 0:
                    result = result * seas[i, x]
                    first[x, t] = result
                    message[x] = jnp.where(mine, result, message[x])
                else:
                    result = pltpu.roll(result, lanes - (2 * i + 1), 1)
                    result = result.astype(f32)
                    for h, part in enumerate(parts):
                        stage[staged(part, x), :] = result[h * HALF : (h + 1) * HALF]
        if e == 0:
            for x in range(rows_x):
                ysend[1, c, x] = message[x]
            start_sends(1, c)

    for c in range(total):
        grow(c)
        if c >= LAG:
            advance(0, c - LAG)
    for c in range(max(total - LAG, 0), total):
        advance(0, c)
    for c in range(total):
        advance(1, c)

    for e in range(PROP):
        for c in range(total):
            for kind in range(4):
                @pl.when(sends[kind])
                def _():
                    exchange(e, c, kind).wait_send()


def flush(rows_x, stage, out_hbm, outv, sem):
    lanes = outv.shape[1]
    length, step = ND * rows_x, pitch(rows_x)
    freqs = outv.shape[0] // length
    pieces = sem.shape[0]
    each = freqs // pieces
    sea = stage[stage.shape[0] - 8 :, :]
    copies = []
    for n in range(pieces):
        for f in range(n * each, (n + 1) * each):
            values = stage[f * step : f * step + length, :].reshape(-1, 8, lanes) * sea[None]
            outv[f * length : (f + 1) * length, :] = values.reshape(length, lanes).astype(outv.dtype)
        part = pl.ds(n * each * length, each * length)
        copy = pltpu.make_async_copy(outv.at[part], out_hbm.at[part], sem.at[n])
        copy.start()
        copies.append(copy)
    for copy in copies:
        copy.wait()


def shards(mesh_counts, spectrum, interaction, speeds, mask):
    comps, rows_x, lanes = spectrum.shape
    chunks = plan(comps)
    total = len(chunks)
    tiles = sum(len(t) for _, _, t, _ in chunks)
    most = max(len(t) for _, _, t, _ in chunks)
    longest = max(end - begin for begin, end, _, _ in chunks)
    any_space = pl.BlockSpec(memory_space=pltpu.HBM)
    vmem = pl.BlockSpec(memory_space=pltpu.VMEM)
    f32, bf16 = jnp.float32, jnp.bfloat16
    freqs = comps // ND
    pieces = next(n for n in range(PIECES, 0, -1) if freqs % n == 0)
    held = -(-(freqs * pitch(rows_x) + SUB * rows_x) // 8) * 8 + 8
    grant = 40 * 1024 * 1024
    pin = functools.partial(pltpu.with_memory_space_constraint, memory_space=pltpu.HBM)
    stage = pl.pallas_call(
        functools.partial(kernel, rows_x, chunks, mesh_counts),
        out_shape=jax.ShapeDtypeStruct((held, lanes), f32),
        in_specs=[any_space] * 4,
        out_specs=vmem,
        scratch_shapes=[
            pltpu.VMEM(speeds.shape, f32),
            pltpu.VMEM(mask.shape, mask.dtype),
            pltpu.VMEM((comps * rows_x, lanes), bf16),
            pltpu.VMEM((comps, comps), bf16),
            pltpu.VMEM((comps, rows_x * lanes), bf16),
            pltpu.VMEM((rows_x, longest + SUB, lanes), f32),
            pltpu.VMEM((rows_x, tiles, SUB, lanes), bf16),
            pltpu.VMEM((rows_x, tiles, SUB, lanes), bf16),
            pltpu.VMEM((comps + SUB, lanes), f32),
            pltpu.VMEM((tiles, 3, SUB, lanes), f32),
            pltpu.VMEM((most, rows_x, SUB, lanes), bf16),
            pltpu.VMEM((PROP, tiles, SUB, lanes), bf16),
            pltpu.VMEM((PROP, total, rows_x, SUB, lanes), bf16),
            pltpu.VMEM((PROP, 2, total, rows_x, SUB, lanes), bf16),
            pltpu.SemaphoreType.DMA((total + 2 + LOADS,)),
            pltpu.SemaphoreType.DMA((PROP, total, 4)),
            pltpu.SemaphoreType.DMA((PROP, total, 4)),
        ],
        compiler_params=pltpu.CompilerParams(
            collective_id=0, has_side_effects=True, vmem_limit_bytes=grant
        ),
    )(pin(spectrum.reshape(comps * rows_x, lanes)), pin(interaction), pin(speeds), pin(mask))
    out = pl.pallas_call(
        functools.partial(flush, rows_x),
        out_shape=jax.ShapeDtypeStruct((comps * rows_x, lanes), bf16),
        in_specs=[vmem],
        out_specs=any_space,
        scratch_shapes=[
            pltpu.VMEM((comps * rows_x, lanes), bf16),
            pltpu.SemaphoreType.DMA((pieces,)),
        ],
        compiler_params=pltpu.CompilerParams(vmem_limit_bytes=12 * 1024 * 1024),
    )(stage)
    return out.reshape(comps, rows_x, lanes)


def solution(mesh):
    placed = (P(None, ("member", "pts"), "sub"), P(), P(), P("pts", "sub"))
    return jax.shard_map(
        functools.partial(shards, (mesh.shape["pts"], mesh.shape["sub"])),
        mesh=mesh,
        in_specs=placed,
        out_specs=P(None, ("member", "pts"), "sub"),
        check_vma=False,
    )
```

```python
import functools
import math

import jax
import jax.numpy as jnp
import numpy as np
from jax import lax
from jax.experimental import pallas as pl
from jax.experimental.pallas import tpu as pltpu
from jax.sharding import PartitionSpec as P

ND = 36
PROP = 2
SUB = 16
HALF = 8
SIZES = (1, 2, 2, 1)
LOADS = 5
PIECES = 10
PAD = 4

coupling = 0.5


def circle():
    angle = np.arange(ND, dtype=np.int32).astype(np.float32) * np.float32(2.0 * math.pi / ND)
    angle = angle.astype(np.float64)
    return np.cos(angle).astype(np.float32), np.sin(angle).astype(np.float32)


def classes():
    cosine, sine = circle()
    key = [(bool(c > 0), bool(s >= 0)) for c, s in zip(cosine, sine)]
    first = next(d for d in range(ND) if key[d][0] and not key[d - 1][0])
    found = []
    for i in range(ND):
        d = (first + i) % ND
        if found and d > 0 and found[-1][0] == key[d]:
            found[-1][1].append(d)
        else:
            found.append((key[d], [d]))
    assert [k[0] for k, _ in found] == sorted((k[0] for k, _ in found), reverse=True)
    return found


def plan(comps):
    freqs = comps // ND
    groups, rest = freqs // HALF, freqs % HALF
    sizes, left = [], groups
    for size in SIZES:
        size = min(size, left)
        if size:
            sizes.append(size)
            left -= size
    while left:
        sizes.insert(1, min(2, left))
        left -= sizes[1]
    chunks, top = [], groups
    for n, size in enumerate(sizes):
        tiles = []
        for g in range(top - size, top):
            for (up_x, up_y), run in classes():
                for pair in [run[i : i + 2] for i in range(0, len(run), 2)]:
                    pair = (pair * 2)[:2]
                    tiles.append(([(g * HALF * ND + d, ND, [d] * HALF) for d in pair], up_x, up_y))
        begin, end = (top - size) * HALF * ND, top * HALF * ND
        if n == 0:
            end = comps
            for f in range(rest):
                for (up_x, up_y), run in sorted(classes(), key=lambda c: c[1][0]):
                    ds = run + [None] * (SUB - len(run))
                    k0 = (groups * HALF + f) * ND + run[0]
                    parts = [(k0, 1, ds[:HALF]), (k0 + HALF, 1, ds[HALF:])]
                    tiles.append((parts, up_x, up_y))
        tiles.sort(key=lambda t: not t[1])
        chunks.append((begin, end, tiles, sum(t[1] for t in tiles)))
        top -= size
    return chunks


def pitch(rows_x):
    step = ND * rows_x + PAD
    return step if step % 8 else step + PAD


def kernel(
    rows_x, chunks, counts,
    spec_hbm, inter_hbm, speeds_hbm, mask_hbm, stage,
    speeds_ref, mask_ref, specv, inter, flat, acc, field, first, column, coefs, seas,
    packed, early, xrecv, ysend, yrecv, corner, own_sea, other_sea,
    load_sem, send_sem, recv_sem, sea_send, sea_recv,
):
    comps, width = flat.shape
    lanes = width // rows_x
    f32, bf16 = jnp.float32, jnp.bfloat16
    px, sy = lax.axis_index("pts"), lax.axis_index("sub")
    nx, ny = counts
    xs, ys = {1: px < nx - 1, -1: px > 0}, {1: sy < ny - 1, -1: sy > 0}
    partner = [{"pts": px + 1}, {"pts": px - 1}, {"sub": sy + 1}, {"sub": sy - 1}]
    sends, receives = [xs[1], xs[-1], ys[1], ys[-1]], [xs[-1], xs[1], ys[-1], ys[1]]
    for dx in (1, -1):
        for dy in (1, -1):
            partner.append({"pts": px + dx, "sub": sy + dy})
            sends.append(jnp.logical_and(xs[dx], ys[dy]))
            receives.append(jnp.logical_and(xs[-dx], ys[-dy]))
    total = len(chunks)
    step = pitch(rows_x)
    bases = list(np.cumsum([0] + [len(tiles) for _, _, tiles, _ in chunks]))

    speeds_copy = pltpu.make_async_copy(speeds_hbm, speeds_ref, load_sem.at[total])
    speeds_copy.start()
    mask_copy = pltpu.make_async_copy(mask_hbm, mask_ref, load_sem.at[total + 1])
    mask_copy.start()
    blocks = comps // (2 * ND)
    loads = next(n for n in range(LOADS, 0, -1) if blocks % n == 0)
    piece = comps * rows_x // loads

    def spec_copy(n):
        part = pl.ds(pl.multiple_of(n * piece, 16), piece)
        return pltpu.make_async_copy(spec_hbm.at[part], specv.at[part], load_sem.at[total + 2 + n])

    for n in range(loads):
        spec_copy(n).start()
    inter_copies = []
    for c, (begin, end, _, _) in enumerate(chunks):
        part = pl.ds(begin, end - begin)
        copy = pltpu.make_async_copy(inter_hbm.at[part], inter.at[part], load_sem.at[c])
        copy.start()
        inter_copies.append(copy)

    barrier = pltpu.get_barrier_semaphore()
    for kind in range(8):
        @pl.when(sends[kind])
        def _():
            pl.semaphore_signal(
                barrier, inc=1, device_id=partner[kind], device_id_type=pl.DeviceIdType.MESH
            )

    def exchange(c, slot):
        _, _, tiles, ups = chunks[c]
        if slot < 4:
            kind = slot % 2
            begin, count = (bases[c], ups) if kind == 0 else (bases[c] + ups, len(tiles) - ups)
            part = pl.ds(begin, count)
            source = field.at[rows_x - 1 if kind == 0 else 0, part] if slot < 2 else early.at[part]
            target = xrecv.at[slot // 2, part]
        elif slot < 6:
            kind = slot - 2
            source, target = ysend.at[c], yrecv.at[kind - 2, c]
        else:
            kind = slot - 2
            source, target = ysend.at[c, 0, rows_x - 1 if kind < 6 else 0], corner.at[kind - 4, c]
        return kind, pltpu.make_async_remote_copy(
            src_ref=source, dst_ref=target,
            send_sem=send_sem.at[c, slot], recv_sem=recv_sem.at[c, slot],
            device_id=partner[kind], device_id_type=pl.DeviceIdType.MESH,
        )

    def send_sea(kind):
        return pltpu.make_async_remote_copy(
            src_ref=own_sea, dst_ref=other_sea.at[kind],
            send_sem=sea_send.at[kind], recv_sem=sea_recv.at[kind],
            device_id=partner[kind], device_id_type=pl.DeviceIdType.MESH,
        )

    def start_sends(c):
        for slot in (4, 5, 6, 7, 8, 9, 0, 1, 2, 3):
            kind, copy = exchange(c, slot)

            @pl.when(sends[kind])
            def _():
                copy.start()

    def wait_receives(c):
        for slot in range(10):
            kind, copy = exchange(c, slot)

            @pl.when(receives[kind])
            def _():
                copy.wait_recv()

    for kind in range(8):
        @pl.when(jnp.logical_not(receives[kind]))
        def _():
            if kind < 4:
                other_sea[kind] = jnp.zeros(other_sea.shape[1:], bf16)
            if kind < 2:
                for c, (_, _, tiles, ups) in enumerate(chunks):
                    begin, end = (0, ups) if kind == 0 else (ups, len(tiles))

                    @pl.loop(bases[c] + begin, bases[c] + end)
                    def _(t):
                        for e in range(2):
                            xrecv[e, t] = jnp.zeros(xrecv.shape[2:], bf16)
            elif kind < 4:
                yrecv[kind - 2] = jnp.zeros(yrecv.shape[1:], bf16)
            else:
                corner[kind - 4] = jnp.zeros(corner.shape[1:], bf16)

    def lane_of(i, up_y):
        return 2 * i if up_y else 2 * i + 1

    speeds_copy.wait()
    mask_copy.wait()

    starts = list(range(0, comps - lanes + 1, lanes))
    for at in starts:
        row = jnp.broadcast_to(speeds_ref[at : at + lanes].reshape(1, lanes), (lanes, lanes))
        column[at : at + lanes, :] = row.T
    done = starts[-1] + lanes
    if done < comps:
        row = jnp.broadcast_to(speeds_ref[done:comps].reshape(1, comps - done), (lanes, comps - done))
        column[done:comps, :] = row.T
    extra = column.shape[0] - comps
    column[comps : comps + extra, :] = jnp.zeros((extra, lanes), f32)
    used = comps // ND * step
    stage[used:, :] = jnp.zeros((stage.shape[0] - used, lanes), f32)
    stage[stage.shape[0] - 8 :, :] = jnp.concatenate(
        [mask_ref[...].astype(f32) * (1.0 / coupling)] * (8 // rows_x), axis=0
    )

    cosine, sine = (np.abs(v) for v in circle())
    row_id = lax.broadcasted_iota(jnp.int32, (HALF, lanes), 0)

    def factor(values, directions):
        found = [float(values[d]) if d is not None else 0.0 for d in directions]
        if len(set(found)) == 1:
            return found[0]
        column = jnp.zeros((HALF, lanes), f32)
        for r, value in enumerate(found):
            column = jnp.where(row_id == r, value, column)
        return column

    lane = lax.broadcasted_iota(jnp.int32, (SUB, lanes), 1)
    lane_f = lane.astype(f32).astype(bf16)
    even = (lane % 2).astype(f32).astype(bf16) == 0.0

    for c, (_, _, tiles, _) in enumerate(chunks):
        together = [jnp.zeros((SUB, lanes), bf16)] * 3
        for i, (parts, _, up_y) in enumerate(tiles):
            mine = lane_f == float(lane_of(i, up_y))
            weights = [[], [], []]
            for h, (k0, stride, directions) in enumerate(parts):
                rows = slice(h * HALF, (h + 1) * HALF)
                speed = column[pl.ds(k0, HALF, stride=stride), :]
                cross, along = speed * factor(cosine, directions), speed * factor(sine, directions)
                for n, value in enumerate((1.0 - cross - along, cross, along)):
                    coefs[bases[c] + i, n, rows] = value
                    weights[n].append(value)
            for n in range(3):
                value = jnp.concatenate(weights[n], axis=0).astype(bf16)
                together[n] = jnp.where(mine, value, together[n])
        for n in range(3):
            packed[c, n] = together[n]

    seaf = [
        jnp.broadcast_to(mask_ref[x : x + 1, :].astype(f32), (SUB, lanes)).astype(bf16)
        for x in range(rows_x)
    ]
    for i in range(seas.shape[0]):
        for x in range(rows_x):
            seas[i, x] = pltpu.roll(seaf[x], 2 * i + 1, 1)

    rows_sea = mask_ref[...].astype(f32)
    own_sea[...] = jnp.concatenate(
        [rows_sea, jnp.zeros((SUB - rows_x, lanes), f32)], axis=0
    ).astype(bf16)
    line = lax.broadcasted_iota(jnp.int32, (1, lanes), 1)

    def splat(row, at):
        value = jnp.sum(jnp.where(line == at, row, 0.0), axis=1, keepdims=True)
        return jnp.broadcast_to(value, (SUB, lanes)).astype(bf16)

    edge_sea = [
        jnp.where(even, splat(rows_sea[x : x + 1], lanes - 1), splat(rows_sea[x : x + 1], 0))
        for x in range(rows_x)
    ]
    for x in range(rows_x):
        packed[total, x] = edge_sea[x]

    small = rows_sea * coupling
    sea_natural = jnp.concatenate([small] * (8 // rows_x), axis=0)

    low = lax.broadcasted_iota(jnp.int32, (8, lanes), 0) < ND % 8
    whole_rows = ND // 8 * 8

    def spread(block):
        length = ND * rows_x
        begin = pl.multiple_of(block * (2 * length), 16)
        home = pl.multiple_of(block * (2 * step), 8)
        values = specv[pl.ds(begin, 2 * length), :].astype(f32)
        values = (values.reshape(-1, 8, lanes) * sea_natural[None]).reshape(2 * length, lanes)
        stage[pl.ds(home, length), :] = values[:length]
        stage[pl.ds(home + step, length), :] = values[length:]
        for x in range(rows_x):
            one = stage[pl.ds(home + x, whole_rows + 8, stride=rows_x), :]
            two = stage[pl.ds(home + step - ND % 8 * rows_x + x, whole_rows + 8, stride=rows_x), :]
            middle = jnp.where(low, one[whole_rows:], two[:8])
            both = jnp.concatenate([one[:whole_rows], middle, two[8:]], axis=0)
            flat[pl.ds(pl.multiple_of(block * (2 * ND), 8), 2 * ND), x * lanes : (x + 1) * lanes] = (
                both.astype(bf16)
            )

    @pl.loop(0, loads)
    def _(n):
        spec_copy(n).wait()
        for i in range(blocks // loads):
            spread(n * (blocks // loads) + i)

    pl.semaphore_wait(barrier, sum(s.astype(jnp.int32) for s in sends))
    for kind in range(4):
        @pl.when(sends[kind])
        def _():
            send_sea(kind).start()

    def staged(part, x):
        k0, stride, _ = part
        begin = k0 // ND * step + k0 % ND * rows_x + x
        return pl.ds(begin, HALF, stride=rows_x if stride == 1 else step)

    def multiply(c):
        begin, end, _, _ = chunks[c]
        inter_copies[c].wait()
        product = jnp.dot(inter[begin:end, :], flat[...], preferred_element_type=f32)
        for x in range(rows_x):
            acc[c % 2, x, 0 : end - begin, :] = product[:, x * lanes : (x + 1) * lanes]

    def below(c):
        return lane_f < float(2 * chunks[c][3])

    def grow(c):
        begin, end, tiles, _ = chunks[c]
        none = jnp.zeros((SUB, lanes), bf16)
        message, second = [none] * rows_x, [none] * rows_x
        for i, (parts, up_x, up_y) in enumerate(tiles):
            t = bases[c] + i
            mine = lane_f == float(lane_of(i, up_y))
            next_lane = lane_f == float((lane_of(i, up_y) + (lanes - 1 if up_y else 1)) % lanes)
            rows = []
            for x in range(rows_x):
                halves = []
                for part in parts:
                    k0, stride, _ = part
                    coupled = acc[c % 2, x, pl.ds(k0 - begin, HALF, stride=stride), :]
                    wide = stage[staged(part, x), :]
                    halves.append(wide + wide * coupled)
                grown = jnp.concatenate(halves, axis=0).astype(bf16)
                grown = pltpu.roll(grown, 2 * i + 1, 1)
                rows.append(grown)
                field[x, t] = grown
                message[x] = jnp.where(mine, grown, message[x])
                second[x] = jnp.where(next_lane, grown, second[x])
            keep, cross, along = (coefs[t, n].astype(bf16) for n in range(3))
            edge, inner = (rows_x - 1, rows_x - 2) if up_x else (0, 1)
            near_y = pltpu.roll(jnp.where(mine, none, rows[edge]), 1 if up_y else lanes - 1, 1)
            result = keep * rows[edge] + cross * rows[inner] + along * near_y
            early[t] = result * seas[i, edge]
        for x in range(rows_x):
            near_y = jnp.where(even, pltpu.roll(second[x], 1, 1), pltpu.roll(second[x], lanes - 1, 1))
            near_x = jnp.where(
                below(c),
                message[x - 1] if x > 0 else none,
                message[x + 1] if x < rows_x - 1 else none,
            )
            result = packed[c, 0] * message[x] + packed[c, 1] * near_x + packed[c, 2] * near_y
            ysend[c, 0, x] = message[x]
            ysend[c, 1, x] = result * packed[total, x]
        start_sends(c)

    def step_one(c):
        _, _, tiles, _ = chunks[c]
        wait_receives(c)
        edges = [jnp.where(even, yrecv[0, c, 0, x], yrecv[1, c, 0, x]) for x in range(rows_x)]
        for i, (_, up_x, up_y) in enumerate(tiles):
            t = bases[c] + i
            mine = lane_f == float(lane_of(i, up_y))
            keep, cross, along = (coefs[t, n].astype(bf16) for n in range(3))
            rows = [field[x, t] for x in range(rows_x)]
            outer = xrecv[0, t]
            for x in range(rows_x):
                if up_x:
                    near_x = rows[x - 1] if x > 0 else outer
                else:
                    near_x = rows[x + 1] if x < rows_x - 1 else outer
                near_y = pltpu.roll(
                    jnp.where(mine, edges[x], rows[x]), 1 if up_y else lanes - 1, 1
                )
                result = keep * rows[x] + cross * near_x + along * near_y
                first[x, t] = result * seas[i, x]

    def neighbours_sea():
        for kind in range(4):
            @pl.when(receives[kind])
            def _():
                send_sea(kind).wait_recv()
        from_low, from_high, from_left, from_right = (
            other_sea[kind].astype(f32) for kind in range(4)
        )
        last = rows_x - 1

        def columns(x):
            return jnp.where(
                even, splat(from_left[x : x + 1], lanes - 1), splat(from_right[x : x + 1], 0)
            )

        packed[total + 1, 0] = columns(0)
        packed[total + 1, 1] = columns(last)
        packed[total + 1, 2] = splat(from_low[last : last + 1], 0)
        packed[total + 1, 3] = splat(from_high[0:1], 0)
        packed[total + 2, 0] = splat(from_low[last : last + 1], lanes - 1)
        packed[total + 2, 1] = splat(from_high[0:1], lanes - 1)

    def step_two(c):
        _, _, tiles, _ = chunks[c]
        low = below(c)
        none = jnp.zeros((SUB, lanes), bf16)
        corners = jnp.where(
            low,
            jnp.where(even, corner[0, c], corner[1, c]),
            jnp.where(even, corner[2, c], corner[3, c]),
        )
        edges = [jnp.where(even, yrecv[0, c, 1, x], yrecv[1, c, 1, x]) for x in range(rows_x)]
        missing = corners * packed[c, 1]
        last = rows_x - 1
        edges[0] = edges[0] + jnp.where(low, missing * packed[total + 1, 0], none)
        edges[last] = edges[last] + jnp.where(low, none, missing * packed[total + 1, 1])
        turned = {
            True: pltpu.roll(corners, 1, 1)
            * jnp.where(low, packed[total + 1, 2], packed[total + 1, 3]),
            False: pltpu.roll(corners, lanes - 1, 1)
            * jnp.where(low, packed[total + 2, 0], packed[total + 2, 1]),
        }
        order = sorted(range(len(tiles)), key=lambda i: (tiles[i][0][0][1] == 1, tiles[i][0][0][0]))
        for i in order:
            parts, up_x, up_y = tiles[i]
            t = bases[c] + i
            mine = lane_f == float(lane_of(i, up_y))
            there = lane_f == float(lane_of(i, not up_y))
            keep, cross, along = (coefs[t, n].astype(bf16) for n in range(3))
            rows = [first[x, t] for x in range(rows_x)]
            outer = jnp.where(there, along * turned[up_y], none) + xrecv[1, t]
            for x in range(rows_x):
                if up_x:
                    near_x = rows[x - 1] if x > 0 else outer
                else:
                    near_x = rows[x + 1] if x < last else outer
                near_y = pltpu.roll(
                    jnp.where(mine, edges[x], rows[x]), 1 if up_y else lanes - 1, 1
                )
                result = keep * rows[x] + cross * near_x + along * near_y
                result = pltpu.roll(result, lanes - (2 * i + 1), 1).astype(f32)
                for h, part in enumerate(parts):
                    stage[staged(part, x), :] = result[h * HALF : (h + 1) * HALF]

    multiply(0)
    for c in range(1, total):
        multiply(c)
        grow(c - 1)
    grow(total - 1)
    neighbours_sea()
    for c in range(total):
        step_one(c)
        step_two(c)

    for kind in range(4):
        @pl.when(sends[kind])
        def _():
            send_sea(kind).wait_send()
    for c in range(total):
        for slot in range(10):
            kind, copy = exchange(c, slot)

            @pl.when(sends[kind])
            def _():
                copy.wait_send()


def flush(rows_x, stage, out_hbm, outv, sem):
    lanes = outv.shape[1]
    length, step = ND * rows_x, pitch(rows_x)
    freqs = outv.shape[0] // length
    pieces = sem.shape[0]
    each = freqs // pieces
    sea = stage[stage.shape[0] - 8 :, :]
    copies = []
    for n in range(pieces):
        for f in range(n * each, (n + 1) * each):
            values = stage[f * step : f * step + length, :].reshape(-1, 8, lanes) * sea[None]
            outv[f * length : (f + 1) * length, :] = values.reshape(length, lanes).astype(outv.dtype)
        part = pl.ds(n * each * length, each * length)
        copy = pltpu.make_async_copy(outv.at[part], out_hbm.at[part], sem.at[n])
        copy.start()
        copies.append(copy)
    for copy in copies:
        copy.wait()


def shards(mesh_counts, spectrum, interaction, speeds, mask):
    comps, rows_x, lanes = spectrum.shape
    chunks = plan(comps)
    total = len(chunks)
    tiles = sum(len(t) for _, _, t, _ in chunks)
    most = max(len(t) for _, _, t, _ in chunks)
    longest = max(end - begin for begin, end, _, _ in chunks)
    any_space = pl.BlockSpec(memory_space=pltpu.HBM)
    vmem = pl.BlockSpec(memory_space=pltpu.VMEM)
    f32, bf16 = jnp.float32, jnp.bfloat16
    freqs = comps // ND
    pieces = next(n for n in range(PIECES, 0, -1) if freqs % n == 0)
    held = -(-(freqs * pitch(rows_x) + SUB * rows_x) // 8) * 8 + 8
    grant = 40 * 1024 * 1024
    pin = functools.partial(pltpu.with_memory_space_constraint, memory_space=pltpu.HBM)
    stage = pl.pallas_call(
        functools.partial(kernel, rows_x, chunks, mesh_counts),
        out_shape=jax.ShapeDtypeStruct((held, lanes), f32),
        in_specs=[any_space] * 4,
        out_specs=vmem,
        scratch_shapes=[
            pltpu.VMEM(speeds.shape, f32),
            pltpu.VMEM(mask.shape, mask.dtype),
            pltpu.VMEM((comps * rows_x, lanes), bf16),
            pltpu.VMEM((comps, comps), bf16),
            pltpu.VMEM((comps, rows_x * lanes), bf16),
            pltpu.VMEM((2, rows_x, longest + SUB, lanes), f32),
            pltpu.VMEM((rows_x, tiles, SUB, lanes), bf16),
            pltpu.VMEM((rows_x, tiles, SUB, lanes), bf16),
            pltpu.VMEM((comps + SUB, lanes), f32),
            pltpu.VMEM((tiles, 3, SUB, lanes), f32),
            pltpu.VMEM((most, rows_x, SUB, lanes), bf16),
            pltpu.VMEM((total + 3, max(rows_x, 4), SUB, lanes), bf16),
            pltpu.VMEM((tiles, SUB, lanes), bf16),
            pltpu.VMEM((PROP, tiles, SUB, lanes), bf16),
            pltpu.VMEM((total, PROP, rows_x, SUB, lanes), bf16),
            pltpu.VMEM((2, total, PROP, rows_x, SUB, lanes), bf16),
            pltpu.VMEM((4, total, SUB, lanes), bf16),
            pltpu.VMEM((SUB, lanes), bf16),
            pltpu.VMEM((4, SUB, lanes), bf16),
            pltpu.SemaphoreType.DMA((total + 2 + LOADS,)),
            pltpu.SemaphoreType.DMA((total, 10)),
            pltpu.SemaphoreType.DMA((total, 10)),
            pltpu.SemaphoreType.DMA((4,)),
            pltpu.SemaphoreType.DMA((4,)),
        ],
        compiler_params=pltpu.CompilerParams(
            collective_id=0, has_side_effects=True, vmem_limit_bytes=grant
        ),
    )(pin(spectrum.reshape(comps * rows_x, lanes)), pin(interaction), pin(speeds), pin(mask))
    out = pl.pallas_call(
        functools.partial(flush, rows_x),
        out_shape=jax.ShapeDtypeStruct((comps * rows_x, lanes), bf16),
        in_specs=[vmem],
        out_specs=any_space,
        scratch_shapes=[
            pltpu.VMEM((comps * rows_x, lanes), bf16),
            pltpu.SemaphoreType.DMA((pieces,)),
        ],
        compiler_params=pltpu.CompilerParams(vmem_limit_bytes=12 * 1024 * 1024),
    )(stage)
    return out.reshape(comps, rows_x, lanes)


def solution(mesh):
    placed = (P(None, ("member", "pts"), "sub"), P(), P(), P("pts", "sub"))
    return jax.shard_map(
        functools.partial(shards, (mesh.shape["pts"], mesh.shape["sub"])),
        mesh=mesh,
        in_specs=placed,
        out_specs=P(None, ("member", "pts"), "sub"),
        check_vma=False,
    )
```

```python
import functools
import math

import jax
import jax.numpy as jnp
import numpy as np
from jax import lax
from jax.experimental import pallas as pl
from jax.experimental.pallas import tpu as pltpu
from jax.sharding import PartitionSpec as P

ND = 36
PROP = 2
SUB = 16
HALF = 8
SIZES = (1, 2, 2, 1)
LOADS = 5
PIECES = 10
PAD = 4

coupling = 0.5


def circle():
    angle = np.arange(ND, dtype=np.int32).astype(np.float32) * np.float32(2.0 * math.pi / ND)
    angle = angle.astype(np.float64)
    return np.cos(angle).astype(np.float32), np.sin(angle).astype(np.float32)


def classes():
    cosine, sine = circle()
    key = [(bool(c > 0), bool(s >= 0)) for c, s in zip(cosine, sine)]
    first = next(d for d in range(ND) if key[d][0] and not key[d - 1][0])
    found = []
    for i in range(ND):
        d = (first + i) % ND
        if found and d > 0 and found[-1][0] == key[d]:
            found[-1][1].append(d)
        else:
            found.append((key[d], [d]))
    assert [k[0] for k, _ in found] == sorted((k[0] for k, _ in found), reverse=True)
    return found


def plan(comps):
    freqs = comps // ND
    groups, rest = freqs // HALF, freqs % HALF
    sizes, left = [], groups
    for size in SIZES:
        size = min(size, left)
        if size:
            sizes.append(size)
            left -= size
    while left:
        sizes.append(min(2, left))
        left -= sizes[-1]
    chunks, low = [], 0
    for n, size in enumerate(sizes):
        tiles = []
        first = low * HALF * ND
        for (up_x, up_y), run in classes():
            if size == 2:
                pairs = [[first + d, first + HALF * ND + d] for d in run]
            else:
                pairs = [
                    ([first + g * HALF * ND + d for d in run[i : i + 2]] * 2)[:2]
                    for g in range(size)
                    for i in range(0, len(run), 2)
                ]
            for pair in pairs:
                tiles.append(([(k0, ND, [k0 % ND] * HALF) for k0 in pair], up_x, up_y))
        low += size
        end = low * HALF * ND
        if n == len(sizes) - 1:
            end = comps
            for f in range(rest):
                for (up_x, up_y), run in sorted(classes(), key=lambda c: c[1][0]):
                    ds = run + [None] * (SUB - len(run))
                    k0 = (groups * HALF + f) * ND + run[0]
                    parts = [(k0, 1, ds[:HALF]), (k0 + HALF, 1, ds[HALF:])]
                    tiles.append((parts, up_x, up_y))
        tiles.sort(key=lambda t: not t[1])
        chunks.append((first, end, tiles, sum(t[1] for t in tiles)))
    return chunks


def pitch(rows_x):
    step = ND * rows_x + PAD
    return step if step % 8 else step + PAD


def kernel(
    rows_x, chunks, counts,
    spec_hbm, inter_hbm, speeds_hbm, mask_hbm, stage,
    speeds_ref, mask_ref, specv, inter, flat, acc, field, first, column, coefs, seas,
    packed, early, xrecv, ysend, yrecv, corner, own_sea, other_sea,
    load_sem, send_sem, recv_sem, sea_send, sea_recv,
):
    comps, width = flat.shape
    lanes = width // rows_x
    f32, bf16 = jnp.float32, jnp.bfloat16
    px, sy = lax.axis_index("pts"), lax.axis_index("sub")
    nx, ny = counts
    xs, ys = {1: px < nx - 1, -1: px > 0}, {1: sy < ny - 1, -1: sy > 0}
    partner = [{"pts": px + 1}, {"pts": px - 1}, {"sub": sy + 1}, {"sub": sy - 1}]
    sends, receives = [xs[1], xs[-1], ys[1], ys[-1]], [xs[-1], xs[1], ys[-1], ys[1]]
    for dx in (1, -1):
        for dy in (1, -1):
            partner.append({"pts": px + dx, "sub": sy + dy})
            sends.append(jnp.logical_and(xs[dx], ys[dy]))
            receives.append(jnp.logical_and(xs[-dx], ys[-dy]))
    total = len(chunks)
    step = pitch(rows_x)
    bases = list(np.cumsum([0] + [len(tiles) for _, _, tiles, _ in chunks]))

    speeds_copy = pltpu.make_async_copy(speeds_hbm, speeds_ref, load_sem.at[total])
    speeds_copy.start()
    mask_copy = pltpu.make_async_copy(mask_hbm, mask_ref, load_sem.at[total + 1])
    mask_copy.start()
    blocks = comps // (2 * ND)
    loads = next(n for n in range(LOADS, 0, -1) if blocks % n == 0)
    piece = comps * rows_x // loads

    def spec_copy(n):
        part = pl.ds(pl.multiple_of(n * piece, 16), piece)
        return pltpu.make_async_copy(spec_hbm.at[part], specv.at[part], load_sem.at[total + 2 + n])

    for n in range(loads):
        spec_copy(n).start()
    inter_copies = []
    for c, (begin, end, _, _) in enumerate(chunks):
        part = pl.ds(begin, end - begin)
        copy = pltpu.make_async_copy(inter_hbm.at[part], inter.at[part], load_sem.at[c])
        copy.start()
        inter_copies.append(copy)

    barrier = pltpu.get_barrier_semaphore()
    for kind in range(8):
        @pl.when(sends[kind])
        def _():
            pl.semaphore_signal(
                barrier, inc=1, device_id=partner[kind], device_id_type=pl.DeviceIdType.MESH
            )

    def exchange(c, slot):
        _, _, tiles, ups = chunks[c]
        if slot < 4:
            kind = slot % 2
            begin, count = (bases[c], ups) if kind == 0 else (bases[c] + ups, len(tiles) - ups)
            part = pl.ds(begin, count)
            source = field.at[rows_x - 1 if kind == 0 else 0, part] if slot < 2 else early.at[part]
            target = xrecv.at[slot // 2, part]
        elif slot < 6:
            kind = slot - 2
            source, target = ysend.at[c], yrecv.at[kind - 2, c]
        else:
            kind = slot - 2
            source, target = ysend.at[c, 0, rows_x - 1 if kind < 6 else 0], corner.at[kind - 4, c]
        return kind, pltpu.make_async_remote_copy(
            src_ref=source, dst_ref=target,
            send_sem=send_sem.at[c, slot], recv_sem=recv_sem.at[c, slot],
            device_id=partner[kind], device_id_type=pl.DeviceIdType.MESH,
        )

    def send_sea(kind):
        return pltpu.make_async_remote_copy(
            src_ref=own_sea, dst_ref=other_sea.at[kind],
            send_sem=sea_send.at[kind], recv_sem=sea_recv.at[kind],
            device_id=partner[kind], device_id_type=pl.DeviceIdType.MESH,
        )

    def start_sends(c):
        for slot in (4, 5, 6, 7, 8, 9, 0, 1, 2, 3):
            kind, copy = exchange(c, slot)

            @pl.when(sends[kind])
            def _():
                copy.start()

    def wait_receives(c):
        for slot in range(10):
            kind, copy = exchange(c, slot)

            @pl.when(receives[kind])
            def _():
                copy.wait_recv()

    for kind in range(8):
        @pl.when(jnp.logical_not(receives[kind]))
        def _():
            if kind < 4:
                other_sea[kind] = jnp.zeros(other_sea.shape[1:], bf16)
            if kind < 2:
                for c, (_, _, tiles, ups) in enumerate(chunks):
                    begin, end = (0, ups) if kind == 0 else (ups, len(tiles))

                    @pl.loop(bases[c] + begin, bases[c] + end)
                    def _(t):
                        for e in range(2):
                            xrecv[e, t] = jnp.zeros(xrecv.shape[2:], bf16)
            elif kind < 4:
                yrecv[kind - 2] = jnp.zeros(yrecv.shape[1:], bf16)
            else:
                corner[kind - 4] = jnp.zeros(corner.shape[1:], bf16)

    def lane_of(i, up_y):
        return 2 * i if up_y else 2 * i + 1

    speeds_copy.wait()
    mask_copy.wait()

    starts = list(range(0, comps - lanes + 1, lanes))
    for at in starts:
        row = jnp.broadcast_to(speeds_ref[at : at + lanes].reshape(1, lanes), (lanes, lanes))
        column[at : at + lanes, :] = row.T
    done = starts[-1] + lanes
    if done < comps:
        row = jnp.broadcast_to(speeds_ref[done:comps].reshape(1, comps - done), (lanes, comps - done))
        column[done:comps, :] = row.T
    extra = column.shape[0] - comps
    column[comps : comps + extra, :] = jnp.zeros((extra, lanes), f32)
    used = comps // ND * step
    stage[used:, :] = jnp.zeros((stage.shape[0] - used, lanes), f32)
    stage[stage.shape[0] - 8 :, :] = jnp.concatenate(
        [mask_ref[...].astype(f32) * (1.0 / coupling)] * (8 // rows_x), axis=0
    )

    cosine, sine = (np.abs(v) for v in circle())
    row_id = lax.broadcasted_iota(jnp.int32, (HALF, lanes), 0)

    def factor(values, directions):
        found = [float(values[d]) if d is not None else 0.0 for d in directions]
        if len(set(found)) == 1:
            return found[0]
        column = jnp.zeros((HALF, lanes), f32)
        for r, value in enumerate(found):
            column = jnp.where(row_id == r, value, column)
        return column

    lane = lax.broadcasted_iota(jnp.int32, (SUB, lanes), 1)
    lane_f = lane.astype(f32).astype(bf16)
    even = (lane % 2).astype(f32).astype(bf16) == 0.0

    for c, (_, _, tiles, _) in enumerate(chunks):
        together = [jnp.zeros((SUB, lanes), bf16)] * 3
        for i, (parts, _, up_y) in enumerate(tiles):
            mine = lane_f == float(lane_of(i, up_y))
            weights = [[], [], []]
            for h, (k0, stride, directions) in enumerate(parts):
                rows = slice(h * HALF, (h + 1) * HALF)
                speed = column[pl.ds(k0, HALF, stride=stride), :]
                cross, along = speed * factor(cosine, directions), speed * factor(sine, directions)
                for n, value in enumerate((1.0 - cross - along, cross, along)):
                    coefs[bases[c] + i, n, rows] = value
                    weights[n].append(value)
            for n in range(3):
                value = jnp.concatenate(weights[n], axis=0).astype(bf16)
                together[n] = jnp.where(mine, value, together[n])
        for n in range(3):
            packed[c, n] = together[n]

    seaf = [
        jnp.broadcast_to(mask_ref[x : x + 1, :].astype(f32), (SUB, lanes)).astype(bf16)
        for x in range(rows_x)
    ]
    for i in range(seas.shape[0]):
        for x in range(rows_x):
            seas[i, x] = pltpu.roll(seaf[x], 2 * i + 1, 1)

    rows_sea = mask_ref[...].astype(f32)
    own_sea[...] = jnp.concatenate(
        [rows_sea, jnp.zeros((SUB - rows_x, lanes), f32)], axis=0
    ).astype(bf16)
    line = lax.broadcasted_iota(jnp.int32, (1, lanes), 1)

    def splat(row, at):
        value = jnp.sum(jnp.where(line == at, row, 0.0), axis=1, keepdims=True)
        return jnp.broadcast_to(value, (SUB, lanes)).astype(bf16)

    edge_sea = [
        jnp.where(even, splat(rows_sea[x : x + 1], lanes - 1), splat(rows_sea[x : x + 1], 0))
        for x in range(rows_x)
    ]
    for x in range(rows_x):
        packed[total, x] = edge_sea[x]

    small = rows_sea * coupling
    sea_natural = jnp.concatenate([small] * (8 // rows_x), axis=0)

    low = lax.broadcasted_iota(jnp.int32, (8, lanes), 0) < ND % 8
    whole_rows = ND // 8 * 8

    def spread(block):
        length = ND * rows_x
        begin = pl.multiple_of(block * (2 * length), 16)
        home = pl.multiple_of(block * (2 * step), 8)
        values = specv[pl.ds(begin, 2 * length), :].astype(f32)
        values = (values.reshape(-1, 8, lanes) * sea_natural[None]).reshape(2 * length, lanes)
        stage[pl.ds(home, length), :] = values[:length]
        stage[pl.ds(home + step, length), :] = values[length:]
        for x in range(rows_x):
            one = stage[pl.ds(home + x, whole_rows + 8, stride=rows_x), :]
            two = stage[pl.ds(home + step - ND % 8 * rows_x + x, whole_rows + 8, stride=rows_x), :]
            middle = jnp.where(low, one[whole_rows:], two[:8])
            both = jnp.concatenate([one[:whole_rows], middle, two[8:]], axis=0)
            flat[pl.ds(pl.multiple_of(block * (2 * ND), 8), 2 * ND), x * lanes : (x + 1) * lanes] = (
                both.astype(bf16)
            )

    @pl.loop(0, loads)
    def _(n):
        spec_copy(n).wait()
        for i in range(blocks // loads):
            spread(n * (blocks // loads) + i)

    def enter():
        pl.semaphore_wait(barrier, sum(s.astype(jnp.int32) for s in sends))
        for kind in range(4):
            @pl.when(sends[kind])
            def _():
                send_sea(kind).start()

    def staged(part, x):
        k0, stride, _ = part
        begin = k0 // ND * step + k0 % ND * rows_x + x
        return pl.ds(begin, HALF, stride=rows_x if stride == 1 else step)

    def multiply(c):
        begin, end, _, _ = chunks[c]
        inter_copies[c].wait()
        product = jnp.dot(inter[begin:end, :], flat[...], preferred_element_type=f32)
        for x in range(rows_x):
            acc[c % 2, x, 0 : end - begin, :] = product[:, x * lanes : (x + 1) * lanes]

    def below(c):
        return lane_f < float(2 * chunks[c][3])

    def grow(c):
        begin, end, tiles, _ = chunks[c]
        none = jnp.zeros((SUB, lanes), bf16)
        message, second = [none] * rows_x, [none] * rows_x
        for i, (parts, up_x, up_y) in enumerate(tiles):
            t = bases[c] + i
            mine = lane_f == float(lane_of(i, up_y))
            next_lane = lane_f == float((lane_of(i, up_y) + (lanes - 1 if up_y else 1)) % lanes)
            rows = []
            for x in range(rows_x):
                halves = []
                for part in parts:
                    k0, stride, _ = part
                    coupled = acc[c % 2, x, pl.ds(k0 - begin, HALF, stride=stride), :]
                    wide = stage[staged(part, x), :]
                    halves.append(wide + wide * coupled)
                grown = jnp.concatenate(halves, axis=0).astype(bf16)
                grown = pltpu.roll(grown, 2 * i + 1, 1)
                rows.append(grown)
                field[x, t] = grown
                message[x] = jnp.where(mine, grown, message[x])
                second[x] = jnp.where(next_lane, grown, second[x])
            keep, cross, along = (coefs[t, n].astype(bf16) for n in range(3))
            edge, inner = (rows_x - 1, rows_x - 2) if up_x else (0, 1)
            near_y = pltpu.roll(jnp.where(mine, none, rows[edge]), 1 if up_y else lanes - 1, 1)
            result = keep * rows[edge] + cross * rows[inner] + along * near_y
            early[t] = result * seas[i, edge]
        for x in range(rows_x):
            near_y = jnp.where(even, pltpu.roll(second[x], 1, 1), pltpu.roll(second[x], lanes - 1, 1))
            near_x = jnp.where(
                below(c),
                message[x - 1] if x > 0 else none,
                message[x + 1] if x < rows_x - 1 else none,
            )
            result = packed[c, 0] * message[x] + packed[c, 1] * near_x + packed[c, 2] * near_y
            ysend[c, 0, x] = message[x]
            ysend[c, 1, x] = result * packed[total, x]
        start_sends(c)

    def step_one(c):
        _, _, tiles, _ = chunks[c]
        wait_receives(c)
        edges = [jnp.where(even, yrecv[0, c, 0, x], yrecv[1, c, 0, x]) for x in range(rows_x)]
        for i, (_, up_x, up_y) in enumerate(tiles):
            t = bases[c] + i
            mine = lane_f == float(lane_of(i, up_y))
            keep, cross, along = (coefs[t, n].astype(bf16) for n in range(3))
            rows = [field[x, t] for x in range(rows_x)]
            outer = xrecv[0, t]
            for x in range(rows_x):
                if up_x:
                    near_x = rows[x - 1] if x > 0 else outer
                else:
                    near_x = rows[x + 1] if x < rows_x - 1 else outer
                near_y = pltpu.roll(
                    jnp.where(mine, edges[x], rows[x]), 1 if up_y else lanes - 1, 1
                )
                result = keep * rows[x] + cross * near_x + along * near_y
                first[x, t] = result * seas[i, x]

    def neighbours_sea():
        for kind in range(4):
            @pl.when(receives[kind])
            def _():
                send_sea(kind).wait_recv()
        from_low, from_high, from_left, from_right = (
            other_sea[kind].astype(f32) for kind in range(4)
        )
        last = rows_x - 1

        def columns(x):
            return jnp.where(
                even, splat(from_left[x : x + 1], lanes - 1), splat(from_right[x : x + 1], 0)
            )

        packed[total + 1, 0] = columns(0)
        packed[total + 1, 1] = columns(last)
        packed[total + 1, 2] = splat(from_low[last : last + 1], 0)
        packed[total + 1, 3] = splat(from_high[0:1], 0)
        packed[total + 2, 0] = splat(from_low[last : last + 1], lanes - 1)
        packed[total + 2, 1] = splat(from_high[0:1], lanes - 1)

    def step_two(c):
        _, _, tiles, _ = chunks[c]
        low = below(c)
        none = jnp.zeros((SUB, lanes), bf16)
        corners = jnp.where(
            low,
            jnp.where(even, corner[0, c], corner[1, c]),
            jnp.where(even, corner[2, c], corner[3, c]),
        )
        edges = [jnp.where(even, yrecv[0, c, 1, x], yrecv[1, c, 1, x]) for x in range(rows_x)]
        missing = corners * packed[c, 1]
        last = rows_x - 1
        edges[0] = edges[0] + jnp.where(low, missing * packed[total + 1, 0], none)
        edges[last] = edges[last] + jnp.where(low, none, missing * packed[total + 1, 1])
        turned = {
            True: pltpu.roll(corners, 1, 1)
            * jnp.where(low, packed[total + 1, 2], packed[total + 1, 3]),
            False: pltpu.roll(corners, lanes - 1, 1)
            * jnp.where(low, packed[total + 2, 0], packed[total + 2, 1]),
        }
        order = sorted(range(len(tiles)), key=lambda i: (tiles[i][0][0][1] == 1, tiles[i][0][0][0]))
        for i in order:
            parts, up_x, up_y = tiles[i]
            t = bases[c] + i
            mine = lane_f == float(lane_of(i, up_y))
            there = lane_f == float(lane_of(i, not up_y))
            keep, cross, along = (coefs[t, n].astype(bf16) for n in range(3))
            rows = [first[x, t] for x in range(rows_x)]
            outer = jnp.where(there, along * turned[up_y], none) + xrecv[1, t]
            for x in range(rows_x):
                if up_x:
                    near_x = rows[x - 1] if x > 0 else outer
                else:
                    near_x = rows[x + 1] if x < last else outer
                near_y = pltpu.roll(
                    jnp.where(mine, edges[x], rows[x]), 1 if up_y else lanes - 1, 1
                )
                result = keep * rows[x] + cross * near_x + along * near_y
                result = pltpu.roll(result, lanes - (2 * i + 1), 1).astype(f32)
                for h, part in enumerate(parts):
                    stage[staged(part, x), :] = result[h * HALF : (h + 1) * HALF]

    multiply(0)
    enter()
    grow(0)
    for c in range(1, total):
        multiply(c)
        grow(c)
    neighbours_sea()
    for c in range(total):
        step_one(c)
        step_two(c)

    for kind in range(4):
        @pl.when(sends[kind])
        def _():
            send_sea(kind).wait_send()
    for c in range(total):
        for slot in range(10):
            kind, copy = exchange(c, slot)

            @pl.when(sends[kind])
            def _():
                copy.wait_send()


def flush(rows_x, stage, out_hbm, outv, sem):
    lanes = outv.shape[1]
    length, step = ND * rows_x, pitch(rows_x)
    freqs = outv.shape[0] // length
    pieces = sem.shape[0]
    each = freqs // pieces
    sea = stage[stage.shape[0] - 8 :, :]
    copies = []
    for n in range(pieces):
        for f in range(n * each, (n + 1) * each):
            values = stage[f * step : f * step + length, :].reshape(-1, 8, lanes) * sea[None]
            outv[f * length : (f + 1) * length, :] = values.reshape(length, lanes).astype(outv.dtype)
        part = pl.ds(n * each * length, each * length)
        copy = pltpu.make_async_copy(outv.at[part], out_hbm.at[part], sem.at[n])
        copy.start()
        copies.append(copy)
    for copy in copies:
        copy.wait()


def shards(mesh_counts, spectrum, interaction, speeds, mask):
    comps, rows_x, lanes = spectrum.shape
    chunks = plan(comps)
    total = len(chunks)
    tiles = sum(len(t) for _, _, t, _ in chunks)
    most = max(len(t) for _, _, t, _ in chunks)
    longest = max(end - begin for begin, end, _, _ in chunks)
    any_space = pl.BlockSpec(memory_space=pltpu.HBM)
    vmem = pl.BlockSpec(memory_space=pltpu.VMEM)
    f32, bf16 = jnp.float32, jnp.bfloat16
    freqs = comps // ND
    pieces = next(n for n in range(PIECES, 0, -1) if freqs % n == 0)
    held = -(-(freqs * pitch(rows_x) + SUB * rows_x) // 8) * 8 + 8
    grant = 40 * 1024 * 1024
    pin = functools.partial(pltpu.with_memory_space_constraint, memory_space=pltpu.HBM)
    stage = pl.pallas_call(
        functools.partial(kernel, rows_x, chunks, mesh_counts),
        out_shape=jax.ShapeDtypeStruct((held, lanes), f32),
        in_specs=[any_space] * 4,
        out_specs=vmem,
        scratch_shapes=[
            pltpu.VMEM(speeds.shape, f32),
            pltpu.VMEM(mask.shape, mask.dtype),
            pltpu.VMEM((comps * rows_x, lanes), bf16),
            pltpu.VMEM((comps, comps), bf16),
            pltpu.VMEM((comps, rows_x * lanes), bf16),
            pltpu.VMEM((2, rows_x, longest + SUB, lanes), f32),
            pltpu.VMEM((rows_x, tiles, SUB, lanes), bf16),
            pltpu.VMEM((rows_x, tiles, SUB, lanes), bf16),
            pltpu.VMEM((comps + SUB, lanes), f32),
            pltpu.VMEM((tiles, 3, SUB, lanes), f32),
            pltpu.VMEM((most, rows_x, SUB, lanes), bf16),
            pltpu.VMEM((total + 3, max(rows_x, 4), SUB, lanes), bf16),
            pltpu.VMEM((tiles, SUB, lanes), bf16),
            pltpu.VMEM((PROP, tiles, SUB, lanes), bf16),
            pltpu.VMEM((total, PROP, rows_x, SUB, lanes), bf16),
            pltpu.VMEM((2, total, PROP, rows_x, SUB, lanes), bf16),
            pltpu.VMEM((4, total, SUB, lanes), bf16),
            pltpu.VMEM((SUB, lanes), bf16),
            pltpu.VMEM((4, SUB, lanes), bf16),
            pltpu.SemaphoreType.DMA((total + 2 + LOADS,)),
            pltpu.SemaphoreType.DMA((total, 10)),
            pltpu.SemaphoreType.DMA((total, 10)),
            pltpu.SemaphoreType.DMA((4,)),
            pltpu.SemaphoreType.DMA((4,)),
        ],
        compiler_params=pltpu.CompilerParams(
            collective_id=0, has_side_effects=True, vmem_limit_bytes=grant
        ),
    )(pin(spectrum.reshape(comps * rows_x, lanes)), pin(interaction), pin(speeds), pin(mask))
    out = pl.pallas_call(
        functools.partial(flush, rows_x),
        out_shape=jax.ShapeDtypeStruct((comps * rows_x, lanes), bf16),
        in_specs=[vmem],
        out_specs=any_space,
        scratch_shapes=[
            pltpu.VMEM((comps * rows_x, lanes), bf16),
            pltpu.SemaphoreType.DMA((pieces,)),
        ],
        compiler_params=pltpu.CompilerParams(vmem_limit_bytes=12 * 1024 * 1024),
    )(stage)
    return out.reshape(comps, rows_x, lanes)


def solution(mesh):
    placed = (P(None, ("member", "pts"), "sub"), P(), P(), P("pts", "sub"))
    return jax.shard_map(
        functools.partial(shards, (mesh.shape["pts"], mesh.shape["sub"])),
        mesh=mesh,
        in_specs=placed,
        out_specs=P(None, ("member", "pts"), "sub"),
        check_vma=False,
    )
```
